32 devices in a mesh: member: 4 (over z), region: 8 (over y, x, core).
Axes of the slice: x: 2, y: 2, z: 4, core: 2. Of those that a mesh axis runs over, the one named last changes fastest.
Arguments:
- background: bfloat16 [64, 13, 192, 1024], P('member', None, 'region'), may hold values from -6 to 6
- obs_ens: bfloat16 [131072, 64], P(('member', 'region')), may hold values from -6 to 6
- obs_value: bfloat16 [131072], P(('member', 'region')), may hold values from -8 to 8
- obs_precision: bfloat16 [131072], P(('member', 'region')), may hold values from 0.0009994507 to 0.0099487305
- obs_row: int32 [131072], P(('member', 'region')), may hold values from 0 to 47
- obs_patch: int32 [131072, 1], P(('member', 'region')), may hold values from 0 to 31; in each aligned block of 4096 rows (0 to 4095, 4096 to 8191, ...) at most 256 rows name the same one
Outputs:
- analysis: bfloat16 [64, 13, 192, 1024], P(None, None, 'member', 'region')
The draws below stay inside these ranges and needn't reach their ends.
Inputs may be any that keep to these rules, and one draw needn't show every extreme that they name: `obs_patch`: among the observations of one device, at most 256 fall in one patch, and some patch receives exactly 256 of them.
All inputs are finite; a program needn't handle non-finite values.
Results may differ from the reference program's by a relative error of at most 0.0015.
The reference program's roundings to bfloat16 on the way count: a program that leaves them out, or rounds other values in their place, can miss the bound.
Values may be sent and summed in bfloat16 or wider, within the bound.
A program may use at most 128 MiB of HBM per device.

```python
import math
import jax
import jax.numpy as jnp
import numpy as np
from jax import lax

K = 64
C = 13
PLAT = 48
PLON = 128
BAND = 2
OBS_DEV = 4096
NS_ITERS = 4
CAP = 256
NPATCH = 32
NLAT = 192
NLON = 1024
NOBS = 131072
N_MEMBER = 4
N_REGION = 8


def place_ends(array, key, low, high):
    place = [jax.random.randint(jax.random.fold_in(key, axis), (), 0, length) for axis, length in enumerate(array.shape)]
    widest = array.shape.index(max(array.shape))
    next_to = place[:widest] + [(place[widest] + 1) % array.shape[widest]] + place[widest + 1:]
    return array.at[tuple(place)].set(low).at[tuple(next_to)].set(high)


def levels(rng, extent, split, smallest, high):
    def one(dim, parts):
        draws = jax.random.uniform(jax.random.fold_in(jax.random.fold_in(rng, 6), dim), (parts,), jnp.float32, smallest / len(split), high / len(split))
        return jnp.repeat(jnp.exp(draws), extent[dim] // parts).reshape((-1,) + (1,) * (len(extent) - dim - 1))

    gain = one(*split[0])
    for cut in split[1:]:
        gain = gain * one(*cut)
    return gain


def assign_block(own_key, own, number, rows, count, top, bound, lean):
    sequence = jax.random.permutation(own_key, count)
    packed, ordinary = shares(count, rows * top, bound, lean, True), shares(count, rows * top, bound, lean, False)
    places = jnp.arange(count)

    def named(tallies, turn):
        used = int((tallies > 0).sum())
        fixed = max(1, used // 4)
        moved = fixed + (places - fixed + turn * (used - fixed)) % max(1, count - fixed)
        return jnp.zeros((count,), jnp.int32).at[sequence[jnp.where(places < fixed, places, moved)]].set(jnp.asarray(tallies, jnp.int32))

    tallies = jnp.where(number % 4 == 0, named(packed, number // 4), named(ordinary, number - number // 4 - 1))
    mixed = jax.random.permutation(jax.random.fold_in(own, 3), count)
    source_of, sink = mixed[0:count // 2 * 2:2], mixed[1:count // 2 * 2:2]
    margin = jnp.minimum(tallies[source_of] - 1, bound - tallies[sink]) // 2
    margin = jnp.where((source_of == sequence[0]) | (sink == sequence[0]) | (tallies[sink] == 0), 0, jnp.maximum(margin, 0))
    moved = jax.random.randint(jax.random.fold_in(own, 4), (count // 2,), 0, 1 << 20) % (margin + 1)
    tallies = tallies.at[source_of].add(-moved).at[sink].add(moved)
    members = jnp.searchsorted(jnp.cumsum(tallies), jnp.arange(rows * top), side="right").astype(jnp.int32)
    table = members.reshape(top, rows).T
    table = table[jax.random.permutation(jax.random.fold_in(own, 1), rows)]
    turn = jax.random.randint(jax.random.fold_in(own, 2), (rows, 1), 0, top)
    return jnp.take_along_axis(table, (jnp.arange(top)[None, :] + turn) % top, axis=1)


def shares(number_of, total, bound, skew, full):
    weights = [(1 << 20) // math.isqrt(grade ** skew) + 1 for grade in range(1, number_of + 1)]
    largest = bound if full else min(bound, max(-(-total // number_of), total * weights[0] // sum(weights)))
    least = 1 if total - largest >= number_of - 1 else 0
    given, rest = [largest] + [least] * (number_of - 1), total - largest - least * (number_of - 1)
    while rest > 0:
        candidates = [i for i in range(1, number_of) if given[i] < largest] or [i for i in range(1, number_of) if given[i] < bound]
        pool, left = sum([weights[i] for i in candidates]), rest
        for i in candidates:
            more = min(bound - given[i], max(1, left * weights[i] // pool), rest)
            given[i] = given[i] + more
            rest = rest - more
    return np.array(given)


def centred(own_key, extent, deviation, most, split=(), kind=jnp.bfloat16):
    gain = levels(own_key, extent, split, -0.22, 0.18) if split else 1.0
    values = jax.random.normal(own_key, extent, jnp.float32) * deviation * gain
    return jnp.minimum(jnp.maximum(values, -most), most).astype(kind)


def setup_inputs(seed: int = 0) -> dict:
    key_list = jax.random.split(jax.random.key(seed), 7)
    background = centred(key_list[0], (K, C, NLAT, NLON), 1.0, 6.0, ((0, 4), (2, 8)))
    obs_ens = centred(key_list[1], (NOBS, K), 1.0, 6.0, ((0, 32),))
    obs_value = centred(key_list[2], (NOBS,), 2.0, 8.0, ((0, 32),))
    obs_precision = jnp.clip(jnp.exp(math.log(0.0099487305) - 2.2979944 * jax.random.uniform(key_list[3], (NOBS,), jnp.float32) ** levels(key_list[3], (NOBS,), ((0, 32),), -0.2, 0.2)), 0.0009994507, 0.0099487305).astype(jnp.bfloat16)
    obs_row = place_ends(jax.random.randint(key_list[4], (NOBS,), 0, PLAT), jax.random.fold_in(key_list[4], 1), 0, PLAT - 1).astype(jnp.int32)
    obs_patch_keys = jax.random.split(jax.random.fold_in(key_list[5], 1), NOBS // OBS_DEV)
    obs_patch_turns = jax.random.permutation(jax.random.fold_in(key_list[5], 3), NOBS // OBS_DEV)
    obs_patch = jax.vmap(lambda own, number: assign_block(jax.random.fold_in(key_list[5], 2), own, number, OBS_DEV, NPATCH, 1, CAP, 1))(obs_patch_keys, obs_patch_turns).reshape((NOBS, 1))
    return {"background": background, "obs_ens": obs_ens, "obs_value": obs_value, "obs_precision": obs_precision, "obs_row": obs_row, "obs_patch": obs_patch}


def batched(left, right):
    return jnp.einsum('bij,bjk->bik', left, right, precision=lax.Precision.HIGHEST)

def localize(row_float, obs_prec):
    centers = jnp.arange(PLAT // BAND, dtype=jnp.float32) * BAND + (BAND - 1) / 2.0
    distance = (row_float[None, :] - centers[:, None]) / (PLAT / 4.0)
    return obs_prec[None, :] * jnp.exp(-0.5 * distance * distance)

def band_transforms(ens_vals, obs_val, obs_prec, row_float):
    ens_float = ens_vals.astype(jnp.float32)
    ens_mean = lax.optimization_barrier(jnp.sum(ens_float, axis=1)) / K
    ens_pert = (ens_float - ens_mean[:, None]).astype(jnp.bfloat16)
    pert_float = ens_pert.astype(jnp.float32)
    innovation = obs_val - ens_mean
    weight = localize(row_float, obs_prec)

    def band_gram(band_weight):
        scaled = (band_weight[:, None] * pert_float).astype(jnp.bfloat16)
        return lax.dot_general(scaled, ens_pert, (((0,), (0,)), ((), ())), preferred_element_type=jnp.float32)
    gram_band = lax.map(band_gram, weight)
    projected = jnp.dot(weight * innovation[None, :], pert_float, precision=lax.Precision.HIGHEST)
    identity = jnp.eye(K, dtype=jnp.float32)
    system = (K - 1.0) * identity + gram_band
    norm_f = jnp.sqrt(lax.optimization_barrier(jnp.sum(system * system, axis=(1, 2))))
    root_iter = system / norm_f[:, None, None]
    inv_root = jnp.broadcast_to(identity, system.shape)
    for newton_step in range(NS_ITERS):
        middle = 1.5 * identity - 0.5 * batched(inv_root, root_iter)
        root_iter = batched(root_iter, middle)
        inv_root = batched(middle, inv_root)
    spread = jnp.sqrt((K - 1.0) / norm_f)[:, None, None] * inv_root
    inverse = batched(inv_root, inv_root) / norm_f[:, None, None]
    mean_shift = jnp.einsum('bjk,bk->bj', inverse, projected, precision=lax.Precision.HIGHEST)
    return (spread + mean_shift[:, :, None]).astype(jnp.bfloat16)

def update(patch_states, transform):
    state_mean = lax.optimization_barrier(jnp.sum(patch_states.astype(jnp.float32), axis=0)) / K
    state_pert = (patch_states.astype(jnp.float32) - state_mean[None]).astype(jnp.bfloat16)
    shaped = state_pert.reshape(K, C, PLAT // BAND, BAND, PLON).astype(jnp.float32)
    increment = jnp.einsum('jcbxl,bjk->kcbxl', shaped, transform.astype(jnp.float32))
    result = state_mean.reshape(1, C, PLAT // BAND, BAND, PLON) + increment
    return result.reshape(K, C, PLAT, PLON).astype(jnp.bfloat16)

def reference(background, obs_ens, obs_value, obs_precision, obs_row, obs_patch):
    target_patch = obs_patch[:, 0].astype(jnp.int32)
    ordering = jnp.argsort(target_patch, stable=True).astype(jnp.int32)
    counts = jax.ops.segment_sum(jnp.ones_like(target_patch), target_patch, NPATCH).astype(jnp.int32)
    starts = (jnp.cumsum(counts) - counts).astype(jnp.int32)
    room = NPATCH * CAP
    padded_order = jnp.concatenate([ordering, jnp.zeros((room,), jnp.int32)])

    def one_patch(patch_id):
        picked = lax.dynamic_slice_in_dim(padded_order, starts[patch_id], room)
        is_live = jnp.arange(room, dtype=jnp.int32) < counts[patch_id]
        ens_vals = jnp.where(is_live[:, None], obs_ens[picked], jnp.zeros((), jnp.bfloat16))
        obs_val = jnp.where(is_live, obs_value[picked].astype(jnp.float32), 0.0)
        obs_prec = jnp.where(is_live, obs_precision[picked].astype(jnp.float32), 0.0)
        row_float = obs_row[picked].astype(jnp.float32)
        transform = band_transforms(ens_vals, obs_val, obs_prec, row_float)
        lat_block = (patch_id // N_REGION).astype(jnp.int32)
        lon_block = (patch_id % N_REGION).astype(jnp.int32)
        zero = jnp.zeros((), jnp.int32)
        patch_states = lax.dynamic_slice(background, (zero, zero, lat_block * PLAT, lon_block * PLON), (K, C, PLAT, PLON))
        return update(patch_states, transform)
    patches = lax.map(one_patch, jnp.arange(NPATCH, dtype=jnp.int32))
    patches = patches.reshape(N_MEMBER, N_REGION, K, C, PLAT, PLON)
    return patches.transpose(2, 3, 0, 4, 1, 5).reshape(K, C, NLAT, NLON)
```

```python
import functools
import math

import jax
import jax.numpy as jnp
from jax import lax
from jax.experimental import pallas as pl
from jax.experimental.pallas import tpu as pltpu
from jax.sharding import PartitionSpec as P

BAND = 2
NS_ITERS = 4
TILE = 8
LANES = 128


def batched(left, right):
    return jnp.einsum("bij,bjk->bik", left, right, precision=lax.Precision.HIGHEST)


def gram_kernel(width, lat_rows, recv_ref, gram_ref, proj_ref, scaled_ref):
    bands = lat_rows // BAND

    @pl.when(pl.program_id(0) == 0)
    def _():
        gram_ref[...] = jnp.zeros_like(gram_ref)
        proj_ref[...] = jnp.zeros_like(proj_ref)

    cols = recv_ref[...].astype(jnp.float32).T
    ens = cols[:width]
    obs_val, obs_prec, row = (cols[width + k : width + k + 1] for k in range(3))
    mean = jnp.sum(ens, axis=0, keepdims=True) / width
    pert = (ens - mean).astype(jnp.bfloat16)
    pert_float = pert.astype(jnp.float32)
    innovation = obs_val - mean
    index = lax.broadcasted_iota(jnp.int32, (bands, 1), 0).astype(jnp.float32)
    distance = (row - (index * BAND + (BAND - 1) / 2.0)) / (lat_rows / 4.0)
    weight = obs_prec * jnp.exp(-0.5 * distance * distance)
    for j in range(bands):
        scaled_ref[j * width : (j + 1) * width, :] = (weight[j : j + 1] * pert_float).astype(
            jnp.bfloat16
        )
    over_obs = (((1,), (1,)), ((), ()))
    gram_ref[...] += lax.dot_general(
        scaled_ref[...], pert, over_obs, preferred_element_type=jnp.float32
    )
    proj_ref[...] += lax.dot_general(
        weight * innovation,
        pert_float,
        over_obs,
        precision=lax.Precision.HIGHEST,
        preferred_element_type=jnp.float32,
    )


def band_grams(recv, width, lat_rows):
    slots, cols = recv.shape
    bands = lat_rows // BAND
    block = math.gcd(slots, 1024)
    gram, projected = pl.pallas_call(
        functools.partial(gram_kernel, width, lat_rows),
        grid=(slots // block,),
        in_specs=[pl.BlockSpec((block, cols), lambda i: (i, 0))],
        out_specs=[
            pl.BlockSpec((bands * width, width), lambda i: (0, 0)),
            pl.BlockSpec((bands, width), lambda i: (0, 0)),
        ],
        out_shape=[
            jax.ShapeDtypeStruct((bands * width, width), jnp.float32),
            jax.ShapeDtypeStruct((bands, width), jnp.float32),
        ],
        scratch_shapes=[pltpu.VMEM((bands * width, block), jnp.bfloat16)],
        compiler_params=pltpu.CompilerParams(vmem_limit_bytes=24 << 20),
        cost_estimate=pl.CostEstimate(
            flops=8 * slots * bands * width * width,
            bytes_accessed=2 * slots * cols,
            transcendentals=slots * bands,
        ),
    )(recv)
    return gram.reshape(bands, width, width), projected


def batched(left, right):
    return jnp.einsum("bij,bjk->bik", left, right, precision=lax.Precision.HIGHEST)


def band_transforms(grams, members):
    gram_band, projected = grams
    identity = jnp.eye(members, dtype=jnp.float32)
    system = (members - 1.0) * identity + gram_band
    norm_f = jnp.sqrt(jnp.sum(system * system, axis=(1, 2)))
    root_iter = system / norm_f[:, None, None]
    inv_root = jnp.broadcast_to(identity, system.shape)
    for newton_step in range(NS_ITERS):
        middle = 1.5 * identity - 0.5 * batched(inv_root, root_iter)
        root_iter = batched(root_iter, middle)
        inv_root = batched(middle, inv_root)
    spread = jnp.sqrt((members - 1.0) / norm_f)[:, None, None] * inv_root
    inverse = batched(inv_root, inv_root) / norm_f[:, None, None]
    mean_shift = jnp.einsum("bjk,bk->bj", inverse, projected, precision=lax.Precision.HIGHEST)
    return (spread + mean_shift[:, :, None]).astype(jnp.bfloat16)


def slot_numbers(target_patch, devices, capacity):
    obs_rows = target_patch.shape[0]
    block = math.gcd(obs_rows, 512)
    nblock = obs_rows // block
    onehot = (target_patch[:, None] == jnp.arange(devices, dtype=jnp.int32)[None, :]).astype(
        jnp.bfloat16
    )
    blocks = onehot.reshape(nblock, block, devices)
    lower = (jnp.arange(block)[:, None] > jnp.arange(block)[None, :]).astype(jnp.bfloat16)
    inner = jnp.einsum("ij,bjd->bid", lower, blocks, preferred_element_type=jnp.float32)
    totals = jnp.sum(blocks, axis=1, dtype=jnp.float32)
    offsets = jnp.cumsum(totals, axis=0) - totals
    before = inner + offsets[:, None, :]
    rank = jnp.sum(before * blocks.astype(jnp.float32), axis=2).reshape(obs_rows).astype(jnp.int32)
    return target_patch * capacity + rank


def dispatch_kernel(slots_ref, packed_ref, out_ref, wide_ref):
    obs_rows = packed_ref.shape[0]
    wide_ref[...] = jnp.zeros_like(wide_ref)
    unroll = math.gcd(obs_rows, 16)

    def place(step, carry):
        for k in range(unroll):
            i = step * unroll + k
            wide_ref[pl.ds(slots_ref[i], 1), :] = packed_ref[pl.ds(i, 1), :]
        return carry

    lax.fori_loop(0, obs_rows // unroll, place, 0)
    out_ref[...] = wide_ref[...].astype(jnp.bfloat16)


def dispatch(slots, packed, total_slots):
    obs_rows, cols = packed.shape
    return pl.pallas_call(
        dispatch_kernel,
        in_specs=[
            pl.BlockSpec(memory_space=pltpu.SMEM),
            pl.BlockSpec(memory_space=pltpu.VMEM),
        ],
        out_specs=pl.BlockSpec(memory_space=pltpu.VMEM),
        out_shape=jax.ShapeDtypeStruct((total_slots, cols), jnp.bfloat16),
        scratch_shapes=[pltpu.VMEM((total_slots, cols), jnp.float32)],
        compiler_params=pltpu.CompilerParams(vmem_limit_bytes=24 << 20),
        cost_estimate=pl.CostEstimate(
            flops=1 << 32, bytes_accessed=8 * obs_rows * cols, transcendentals=0
        ),
    )(slots, packed)


def exchange_kernel(
    members, regions, bg_ref, obs_ref, recv_ref, got_ref, held_ref,
    local_sem, spread_send, spread_recv, lift_send, lift_recv, out_sem, obs_send, obs_recv, obs_local,
):
    strips = regions // members
    devices = members * regions
    channels = bg_ref.shape[1]
    m, r = lax.axis_index("member"), lax.axis_index("region")
    me = m * regions + r
    barrier = pltpu.get_barrier_semaphore()

    def greet(d, carry):
        other = lax.rem(me + d, devices)
        where = {"member": lax.div(other, regions), "region": lax.rem(other, regions)}
        pl.semaphore_signal(barrier, inc=1, device_id=where, device_id_type=pl.DeviceIdType.MESH)
        return carry

    lax.fori_loop(1, devices, greet, 0)
    pl.semaphore_wait(barrier, devices - 1)

    slot = jnp.where(
        lax.div(r, strips) == m, m * strips + lax.rem(r, strips), members * strips + r
    )

    def block(c, b):
        return bg_ref.at[:, c, :, pl.ds(pl.multiple_of(b * LANES, LANES), LANES)]

    for c in range(channels):

        def spread(d, carry, c=c):
            b = lax.rem(r + d, regions)
            pltpu.make_async_remote_copy(
                block(c, b), held_ref.at[slot, c], spread_send.at[c], spread_recv.at[c],
                device_id={"region": b}, device_id_type=pl.DeviceIdType.MESH,
            ).start()
            return carry

        lax.fori_loop(1, regions, spread, 0)
        pltpu.make_async_copy(block(c, r), held_ref.at[slot, c], local_sem.at[c]).start()

    def send_obs(d, carry):
        other = lax.rem(me + d, devices)
        where = {"member": lax.div(other, regions), "region": lax.rem(other, regions)}
        pltpu.make_async_remote_copy(
            obs_ref.at[other], got_ref.at[me], obs_send, obs_recv,
            device_id=where, device_id_type=pl.DeviceIdType.MESH,
        ).start()
        return carry

    lax.fori_loop(1, devices, send_obs, 0)
    pltpu.make_async_copy(obs_ref.at[me], got_ref.at[me], obs_local).start()

    lifted = (members - 1) * strips
    for c in range(channels):
        pltpu.make_async_copy(held_ref.at[0, c], held_ref.at[0, c], local_sem.at[c]).wait()
        spread_all = held_ref.at[0 : regions - 1, c]
        pltpu.make_async_copy(spread_all, spread_all, spread_recv.at[c]).wait()
        for s in range(members - 1, 0, -1):
            a = lax.rem(m + s, members)
            for j in range(strips):
                pltpu.make_async_remote_copy(
                    held_ref.at[members * strips + a * strips + j, c],
                    held_ref.at[m * strips + j, c],
                    lift_send.at[c], lift_recv.at[c],
                    device_id={"member": a}, device_id_type=pl.DeviceIdType.MESH,
                ).start()
    for c in range(channels):
        lift_all = held_ref.at[0:lifted, c]
        pltpu.make_async_copy(lift_all, lift_all, lift_recv.at[c]).wait()
        pltpu.make_async_copy(
            held_ref.at[0 : members * strips, c], recv_ref.at[:, c], out_sem.at[c]
        ).start()
    for c in range(channels):
        spread_all = held_ref.at[0 : regions - 1, c]
        pltpu.make_async_copy(spread_all, spread_all, spread_send.at[c]).wait()
        lift_all = held_ref.at[0:lifted, c]
        pltpu.make_async_copy(lift_all, lift_all, lift_send.at[c]).wait()
        pltpu.make_async_copy(
            held_ref.at[0 : members * strips, c], recv_ref.at[:, c], out_sem.at[c]
        ).wait()
    obs_all = got_ref.at[0 : devices - 1]
    pltpu.make_async_copy(obs_all, obs_all, obs_send).wait()
    pltpu.make_async_copy(obs_all, obs_all, obs_recv).wait()
    pltpu.make_async_copy(obs_ref.at[0], got_ref.at[0], obs_local).wait()


def exchange(background, buffer):
    members, regions = lax.axis_size("member"), lax.axis_size("region")
    strips = regions // members
    local_members, channels, rows, _ = background.shape
    dma = pltpu.SemaphoreType.DMA
    return pl.pallas_call(
        functools.partial(exchange_kernel, members, regions),
        in_specs=[pl.BlockSpec(memory_space=pl.ANY)] * 2,
        out_specs=[pl.BlockSpec(memory_space=pl.ANY)] * 2,
        out_shape=[
            jax.ShapeDtypeStruct(
                (members * strips, channels, local_members, rows, LANES), background.dtype
            ),
            jax.ShapeDtypeStruct(buffer.shape, buffer.dtype),
        ],
        scratch_shapes=[
            pltpu.VMEM(
                (members * strips + regions, channels, local_members, rows, LANES),
                background.dtype,
            )
        ]
        + [dma((channels,))] * 6
        + [dma, dma, dma],
        compiler_params=pltpu.CompilerParams(
            collective_id=0, has_side_effects=True, vmem_limit_bytes=60 << 20
        ),
    )(background, buffer)


def apply_kernel(members, transform_ref, recv_ref, out_ref, wide_ref):
    slots, block, local_members, rows, lanes = recv_ref.shape
    strips = slots // members
    width = members * local_members
    side = width * TILE
    tiles = rows // TILE

    @pl.when(pl.program_id(0) == 0)
    def _():
        long = lax.broadcasted_iota(jnp.int32, (side, width), 0)
        repeat = (long // TILE == lax.broadcasted_iota(jnp.int32, (side, width), 1)).astype(
            jnp.bfloat16
        )
        row = lax.broadcasted_iota(jnp.int32, (side, side), 0) % TILE
        col = lax.broadcasted_iota(jnp.int32, (side, side), 1) % TILE
        same = row == col
        for t in range(strips * tiles):
            picked = jnp.zeros((side, width), jnp.float32)
            for j in range(TILE // BAND):
                band = transform_ref[t * (TILE // BAND) + j]
                tall = lax.dot_general(
                    repeat, band, (((1,), (1,)), ((), ())), preferred_element_type=jnp.float32
                )
                picked = jnp.where(long % TILE // BAND == j, tall, picked)
            spread = lax.dot_general(
                picked.astype(jnp.bfloat16),
                repeat,
                (((1,), (1,)), ((), ())),
                preferred_element_type=jnp.float32,
            )
            wide_ref[t] = jnp.where(same, spread, 0.0).astype(jnp.bfloat16)

    for j in range(strips):
        for t in range(tiles):
            means, perts = [], []
            for c in range(block):
                state = jnp.concatenate(
                    [
                        recv_ref[m * strips + j, c, :, t * TILE : (t + 1) * TILE, :]
                        for m in range(members)
                    ],
                    axis=0,
                ).astype(jnp.float32)
                mean = jnp.sum(state, axis=0) / width
                means.append(mean)
                perts.append((state - mean[None]).reshape(side, lanes).astype(jnp.bfloat16))
            gain = jnp.dot(
                wide_ref[j * tiles + t],
                jnp.concatenate(perts, axis=1),
                preferred_element_type=jnp.float32,
            )
            for c in range(block):
                one = gain[:, c * lanes : (c + 1) * lanes].reshape(width, TILE, lanes)
                first = j * rows + t * TILE
                out_ref[:, c, first : first + TILE, :] = (one + means[c][None]).astype(
                    jnp.bfloat16
                )


def apply_transform(recv, transform, members):
    slots, channels, local_members, rows, lanes = recv.shape
    strips = slots // members
    width = members * local_members
    if rows % TILE:
        states = recv.reshape(members, strips, channels, local_members, rows, lanes)
        mean = jnp.sum(states, axis=(0, 3), dtype=jnp.float32) / width
        pert = (states.astype(jnp.float32) - mean[None, :, :, None]).astype(jnp.bfloat16)
        gains = jnp.repeat(transform, BAND, axis=0).reshape(
            strips, rows, members, local_members, width
        )
        gain = jnp.einsum(
            "mrjnxl,rxmnk->kjrxl", pert.transpose(0, 1, 2, 3, 4, 5), gains,
            preferred_element_type=jnp.float32,
        )
        out = mean.transpose(1, 0, 2, 3)[None] + gain
        return out.reshape(width, channels, strips * rows, lanes).astype(jnp.bfloat16)
    block = 2
    return pl.pallas_call(
        functools.partial(apply_kernel, members),
        grid=(pl.cdiv(channels, block),),
        in_specs=[
            pl.BlockSpec(transform.shape, lambda i: (0, 0, 0)),
            pl.BlockSpec((slots, block, local_members, rows, lanes), lambda i: (0, i, 0, 0, 0)),
        ],
        out_specs=pl.BlockSpec((width, block, strips * rows, lanes), lambda i: (0, i, 0, 0)),
        out_shape=jax.ShapeDtypeStruct((width, channels, strips * rows, lanes), jnp.bfloat16),
        scratch_shapes=[
            pltpu.VMEM((strips * rows // TILE, width * TILE, width * TILE), jnp.bfloat16)
        ],
        compiler_params=pltpu.CompilerParams(vmem_limit_bytes=32 << 20),
    )(transform, recv)


def local(background, obs_ens, obs_value, obs_precision, obs_row, obs_patch):
    members = lax.axis_size("member")
    regions = lax.axis_size("region")
    devices = members * regions
    obs_rows = obs_row.shape[0]
    capacity = 2 * obs_rows // devices
    total_slots = devices * capacity
    width = obs_ens.shape[1]
    target_patch = obs_patch[:, 0]
    slots = slot_numbers(target_patch, devices, capacity)
    packed_cols = (width + 3 + 127) // 128 * 128
    extras = jnp.stack([obs_value, obs_precision, obs_row.astype(jnp.bfloat16)], axis=1)
    filler = jnp.zeros((obs_rows, packed_cols - width - 3), jnp.bfloat16)
    packed = jnp.concatenate([obs_ens, extras, filler], axis=1)
    buffer = dispatch(slots, packed.astype(jnp.float32), total_slots)
    recv, got = exchange(background, buffer.reshape(devices, capacity, packed_cols))
    lat_rows = (regions // members) * background.shape[2]
    grams = band_grams(got.reshape(total_slots, packed_cols), width, lat_rows)
    transform = band_transforms(grams, width)
    return apply_transform(recv, transform, members)


def solution(mesh):
    in_specs = (
        P("member", None, "region", None),
        P(("member", "region"), None),
        P(("member", "region")),
        P(("member", "region")),
        P(("member", "region")),
        P(("member", "region"), None),
    )
    out_specs = P(None, None, "member", "region")
    return jax.shard_map(
        local, mesh=mesh, in_specs=in_specs, out_specs=out_specs, check_vma=False
    )
```

```python
import functools
import math

import jax
import jax.numpy as jnp
from jax import lax
from jax.experimental import pallas as pl
from jax.experimental.pallas import tpu as pltpu
from jax.sharding import PartitionSpec as P


BAND = 2
NS_ITERS = 4
TILE = 8
LANES = 128
LATE = 3
EXTRAS = 8
MESH = pl.DeviceIdType.MESH


def exchange_kernel(
    members, regions, late, bg_ref, ens_ref, extras_ref, *refs
):
    strips = regions // members
    devices = members * regions
    channels = bg_ref.shape[1]
    early = channels - late
    recv_ref, own_ref = refs[:2]
    lift_refs = refs[2 : 1 + members]
    got_ref = refs[1 + members]
    (
        held_ref, packed_ref, extra_ref, rank_ref, obs_ref,
        local_sem, spread_send, spread_recv, lift_send, lift_recv, out_sem,
        in_sem, obs_sem,
    ) = refs[2 + members :]
    width, obs_rows = ens_ref.shape
    capacity = obs_ref.shape[2]
    m, r = lax.axis_index("member"), lax.axis_index("region")
    me = m * regions + r
    first_stage = members * strips

    ens_copy = pltpu.make_async_copy(ens_ref, packed_ref.at[0:width], in_sem.at[0])
    extra_copy = pltpu.make_async_copy(extras_ref, extra_ref, in_sem.at[1])
    ens_copy.start()
    extra_copy.start()
    barrier = pltpu.get_barrier_semaphore()

    def at_device(other):
        return {"member": lax.div(other, regions), "region": lax.rem(other, regions)}

    def greet(d, carry):
        other = lax.rem(me + d, devices)
        pl.semaphore_signal(
            barrier, inc=1, device_id=at_device(other), device_id_type=MESH
        )
        return carry

    lax.fori_loop(1, devices, greet, 0)
    pl.semaphore_wait(barrier, devices - 1)

    slot = jnp.where(lax.div(r, strips) == m, lax.rem(r, strips), first_stage + r)

    def block(c, b):
        return bg_ref.at[:, c, :, pl.ds(pl.multiple_of(b * LANES, LANES), LANES)]

    for c in range(channels):

        def spread(d, carry, c=c):
            b = lax.rem(r + d, regions)
            pltpu.make_async_remote_copy(
                block(c, b), held_ref.at[slot, c], spread_send.at[c], spread_recv.at[c],
                device_id={"region": b}, device_id_type=MESH,
            ).start()
            return carry

        lax.fori_loop(1, regions, spread, 0)
        pltpu.make_async_copy(block(c, r), held_ref.at[slot, c], local_sem.at[c]).start()

    lifted = (members - 1) * strips
    shifts = range(members - 1, 0, -1)

    def arrive(c):
        pltpu.make_async_copy(held_ref.at[0, c], held_ref.at[0, c], local_sem.at[c]).wait()
        spread_all = held_ref.at[0 : regions - 1, c]
        pltpu.make_async_copy(spread_all, spread_all, spread_recv.at[c]).wait()

    def forward(c):
        arrive(c)
        for s in shifts:
            a = lax.rem(m + s, members)
            for j in range(strips):
                pltpu.make_async_remote_copy(
                    held_ref.at[first_stage + a * strips + j, c],
                    held_ref.at[s * strips + j, c],
                    lift_send.at[c], lift_recv.at[c],
                    device_id={"member": a}, device_id_type=MESH,
                ).start()

    ens_copy.wait()
    extra_copy.wait()
    packed_ref[width:, :] = extra_ref[...].astype(jnp.bfloat16)
    chunk = math.gcd(obs_rows, 512)
    upper = (
        lax.broadcasted_iota(jnp.int32, (chunk, chunk), 0)
        < lax.broadcasted_iota(jnp.int32, (chunk, chunk), 1)
    ).astype(jnp.bfloat16)
    names = lax.broadcasted_iota(jnp.int32, (devices, 1), 0).astype(jnp.float32)
    offset = jnp.zeros((devices, 1), jnp.float32)
    for k in range(obs_rows // chunk):
        span = slice(k * chunk, (k + 1) * chunk)
        hit = extra_ref[3:4, span] == names
        one = hit.astype(jnp.float32)
        before = offset + jnp.dot(
            one.astype(jnp.bfloat16), upper, preferred_element_type=jnp.float32
        )
        rank_ref[:, span] = jnp.sum(jnp.where(hit, before, 0.0), axis=0, keepdims=True)
        offset = offset + jnp.sum(one, axis=1, keepdims=True)
    places = lax.broadcasted_iota(jnp.int32, (capacity, 1), 0).astype(jnp.float32)

    def place(d, carry):
        total = jnp.zeros((width + EXTRAS, capacity), jnp.float32)
        for k in range(obs_rows // chunk):
            span = slice(k * chunk, (k + 1) * chunk)
            mine = jnp.where(
                extra_ref[3:4, span] == d.astype(jnp.float32), rank_ref[:, span], -1.0
            )
            pick = (places == mine).astype(jnp.float32).astype(jnp.bfloat16)
            total = total + lax.dot_general(
                packed_ref[:, span], pick, (((1,), (1,)), ((), ())),
                preferred_element_type=jnp.float32,
            )
        obs_ref[d] = total.astype(jnp.bfloat16)
        return carry

    stages = min(4, early - 1)
    for k in range(stages):
        forward(k)
        lax.fori_loop(devices * k // stages, devices * (k + 1) // stages, place, 0)
    forward(stages)

    def send_obs(d, carry):
        other = lax.rem(me + d, devices)
        pltpu.make_async_remote_copy(
            obs_ref.at[other], got_ref.at[me], obs_sem.at[0], obs_sem.at[1],
            device_id=at_device(other), device_id_type=MESH,
        ).start()
        return carry

    lax.fori_loop(1, devices, send_obs, 0)
    pltpu.make_async_copy(obs_ref.at[me], got_ref.at[me], obs_sem.at[2]).start()
    for c in range(stages + 1, early):
        forward(c)

    def late_copies(c):
        copies = [pltpu.make_async_copy(held_ref.at[0:strips, c], own_ref.at[:, c - early], out_sem.at[c, 0])]
        for s in range(1, members):
            a = lax.rem(m + s, members)
            copies.append(
                pltpu.make_async_copy(
                    held_ref.at[pl.ds(first_stage + a * strips, strips), c],
                    lift_refs[s - 1].at[:, c - early],
                    out_sem.at[c, s],
                )
            )
        return copies

    for c in range(early, channels):
        arrive(c)
        for copy in late_copies(c):
            copy.start()

    def early_copy(c):
        return pltpu.make_async_copy(
            held_ref.at[0:first_stage, c], recv_ref.at[:, c], out_sem.at[c, 0]
        )

    for c in range(early):
        lift_all = held_ref.at[0:lifted, c]
        pltpu.make_async_copy(lift_all, lift_all, lift_recv.at[c]).wait()
        early_copy(c).start()
    for c in range(channels):
        spread_all = held_ref.at[0 : regions - 1, c]
        pltpu.make_async_copy(spread_all, spread_all, spread_send.at[c]).wait()
    obs_all = got_ref.at[0 : devices - 1]
    pltpu.make_async_copy(obs_all, obs_all, obs_sem.at[0]).wait()
    pltpu.make_async_copy(obs_all, obs_all, obs_sem.at[1]).wait()
    pltpu.make_async_copy(obs_ref.at[0], got_ref.at[0], obs_sem.at[2]).wait()
    for c in range(early, channels):
        for copy in late_copies(c):
            copy.wait()
    for c in range(early):
        lift_all = held_ref.at[0:lifted, c]
        pltpu.make_async_copy(lift_all, lift_all, lift_send.at[c]).wait()
        early_copy(c).wait()


def exchange(background, ens_cols, extras, capacity):
    members, regions = lax.axis_size("member"), lax.axis_size("region")
    strips = regions // members
    devices = members * regions
    local_members, channels, rows, _ = background.shape
    width, obs_rows = ens_cols.shape
    late = min(LATE, channels - 2)
    dma = pltpu.SemaphoreType.DMA
    kind = background.dtype
    part = jax.ShapeDtypeStruct((strips, late, local_members, rows, LANES), kind)
    out = pl.pallas_call(
        functools.partial(exchange_kernel, members, regions, late),
        in_specs=[pl.BlockSpec(memory_space=pl.ANY)] * 3,
        out_specs=[pl.BlockSpec(memory_space=pl.ANY)] * (members + 2),
        out_shape=[
            jax.ShapeDtypeStruct(
                (members * strips, channels - late, local_members, rows, LANES), kind
            )
        ]
        + [part] * members
        + [jax.ShapeDtypeStruct((devices, width + EXTRAS, capacity), jnp.bfloat16)],
        scratch_shapes=[
            pltpu.VMEM(
                (members * strips + regions, channels, local_members, rows, LANES), kind
            ),
            pltpu.VMEM((width + EXTRAS, obs_rows), jnp.bfloat16),
            pltpu.VMEM((EXTRAS, obs_rows), jnp.float32),
            pltpu.VMEM((1, obs_rows), jnp.float32),
            pltpu.VMEM((devices, width + EXTRAS, capacity), jnp.bfloat16),
        ]
        + [dma((channels,))] * 5
        + [dma((channels, members)), dma((2,)), dma((3,))],
        compiler_params=pltpu.CompilerParams(
            collective_id=0, has_side_effects=True, vmem_limit_bytes=60 << 20
        ),
        cost_estimate=pl.CostEstimate(
            flops=1 << 34, bytes_accessed=4 * background.size, transcendentals=0
        ),
    )(background, ens_cols, extras)
    return out[0], list(out[1 : 1 + members]), out[1 + members]


def gram_kernel(width, lat_rows, got_ref, gram_ref, proj_ref, scaled_ref):
    bands = lat_rows // BAND

    @pl.when(pl.program_id(0) == 0)
    def _():
        gram_ref[...] = jnp.zeros_like(gram_ref)
        proj_ref[...] = jnp.zeros_like(proj_ref)

    cols = jnp.concatenate(
        [got_ref[k].astype(jnp.float32) for k in range(got_ref.shape[0])], axis=1
    )
    ens = cols[:width]
    obs_val, obs_prec, row = (cols[width + k : width + k + 1] for k in range(3))
    mean = jnp.sum(ens, axis=0, keepdims=True) / width
    pert = (ens - mean).astype(jnp.bfloat16)
    pert_float = pert.astype(jnp.float32)
    innovation = obs_val - mean
    index = lax.broadcasted_iota(jnp.int32, (bands, 1), 0).astype(jnp.float32)
    distance = (row - (index * BAND + (BAND - 1) / 2.0)) / (lat_rows / 4.0)
    weight = obs_prec * jnp.exp(-0.5 * distance * distance)
    for j in range(bands):
        scaled_ref[j * width : (j + 1) * width, :] = (weight[j : j + 1] * pert_float).astype(
            jnp.bfloat16
        )
    over_obs = (((1,), (1,)), ((), ()))
    gram_ref[...] += lax.dot_general(
        scaled_ref[...], pert, over_obs, preferred_element_type=jnp.float32
    )
    proj_ref[...] += lax.dot_general(
        weight * innovation,
        pert_float,
        over_obs,
        precision=lax.Precision.HIGHEST,
        preferred_element_type=jnp.float32,
    )


def band_grams(got, width, lat_rows):
    devices, cols, capacity = got.shape
    bands = lat_rows // BAND
    group = max(1, math.gcd(devices, 1024 // capacity))
    gram, projected = pl.pallas_call(
        functools.partial(gram_kernel, width, lat_rows),
        grid=(devices // group,),
        in_specs=[pl.BlockSpec((group, cols, capacity), lambda i: (i, 0, 0))],
        out_specs=[
            pl.BlockSpec((bands * width, width), lambda i: (0, 0)),
            pl.BlockSpec((bands, width), lambda i: (0, 0)),
        ],
        out_shape=[
            jax.ShapeDtypeStruct((bands * width, width), jnp.float32),
            jax.ShapeDtypeStruct((bands, width), jnp.float32),
        ],
        scratch_shapes=[pltpu.VMEM((bands * width, group * capacity), jnp.bfloat16)],
        compiler_params=pltpu.CompilerParams(vmem_limit_bytes=24 << 20),
        cost_estimate=pl.CostEstimate(
            flops=8 * devices * capacity * bands * width * width,
            bytes_accessed=2 * devices * capacity * cols,
            transcendentals=devices * capacity * bands,
        ),
    )(got)
    return gram.reshape(bands, width, width), projected


def batched(left, right):
    return jnp.einsum("bij,bjk->bik", left, right, precision=lax.Precision.HIGHEST)


def band_transforms(grams, members):
    gram_band, projected = grams
    identity = jnp.eye(members, dtype=jnp.float32)
    system = (members - 1.0) * identity + gram_band
    norm_f = jnp.sqrt(jnp.sum(system * system, axis=(1, 2)))
    root_iter = system / norm_f[:, None, None]
    inv_root = jnp.broadcast_to(identity, system.shape)
    for _ in range(NS_ITERS):
        middle = 1.5 * identity - 0.5 * batched(inv_root, root_iter)
        root_iter = batched(root_iter, middle)
        inv_root = batched(middle, inv_root)
    spread = jnp.sqrt((members - 1.0) / norm_f)[:, None, None] * inv_root
    inverse = batched(inv_root, inv_root) / norm_f[:, None, None]
    mean_shift = jnp.einsum("bjk,bk->bj", inverse, projected, precision=lax.Precision.HIGHEST)
    return (spread + mean_shift[:, :, None]).astype(jnp.bfloat16)


def widen_kernel(transform_ref, wide_ref, turned_ref):
    bands, members, _, width = transform_ref.shape
    side = width * TILE
    m = lax.axis_index("member")
    for s in range(members):
        turned_ref[:, s] = transform_ref[:, lax.rem(m - s + members, members)]
    long = lax.broadcasted_iota(jnp.int32, (side, width), 0)
    repeat = (long // TILE == lax.broadcasted_iota(jnp.int32, (side, width), 1)).astype(
        jnp.bfloat16
    )
    row = lax.broadcasted_iota(jnp.int32, (side, side), 0) % TILE
    col = lax.broadcasted_iota(jnp.int32, (side, side), 1) % TILE
    same = row == col
    over_last = (((1,), (1,)), ((), ()))
    for t in range(bands * BAND // TILE):
        picked = jnp.zeros((side, width), jnp.float32)
        for j in range(TILE // BAND):
            band = turned_ref[t * (TILE // BAND) + j].reshape(width, width)
            tall = lax.dot_general(repeat, band, over_last, preferred_element_type=jnp.float32)
            picked = jnp.where(long % TILE // BAND == j, tall, picked)
        spread = lax.dot_general(
            picked.astype(jnp.bfloat16), repeat, over_last, preferred_element_type=jnp.float32
        )
        wide_ref[t] = jnp.where(same, spread, 0.0).astype(jnp.bfloat16)


def widen(transform, members):
    bands, width, _ = transform.shape
    side = width * TILE
    return pl.pallas_call(
        widen_kernel,
        in_specs=[pl.BlockSpec(memory_space=pltpu.VMEM)],
        out_specs=pl.BlockSpec(memory_space=pltpu.VMEM),
        out_shape=jax.ShapeDtypeStruct((bands * BAND // TILE, side, side), jnp.bfloat16),
        scratch_shapes=[pltpu.VMEM((bands, members, width // members, width), jnp.bfloat16)],
        compiler_params=pltpu.CompilerParams(vmem_limit_bytes=24 << 20),
        cost_estimate=pl.CostEstimate(
            flops=1 << 31, bytes_accessed=8 * side * side, transcendentals=0
        ),
    )(transform.reshape(bands, members, width // members, width))


def apply_kernel(members, pieces, wide_ref, *refs):
    parts, out_ref = refs[:pieces], refs[-1]
    slots, block, local_members, rows, lanes = parts[0].shape
    strips = slots * pieces // members
    width = members * local_members
    side = width * TILE
    tiles = rows // TILE
    for j in range(strips):
        for t in range(tiles):
            means, perts = [], []
            for c in range(block):
                states = []
                for s in range(members):
                    place = s * strips + j
                    ref = parts[place // slots]
                    states.append(
                        ref[place % slots, c, :, t * TILE : (t + 1) * TILE, :].astype(
                            jnp.float32
                        )
                    )
                state = jnp.concatenate(states, axis=0)
                mean = jnp.sum(state, axis=0) / width
                means.append(mean)
                perts.append((state - mean[None]).reshape(side, lanes).astype(jnp.bfloat16))
            gain = jnp.dot(
                wide_ref[j * tiles + t],
                jnp.concatenate(perts, axis=1),
                preferred_element_type=jnp.float32,
            )
            for c in range(block):
                one = gain[:, c * lanes : (c + 1) * lanes].reshape(width, TILE, lanes)
                first = j * rows + t * TILE
                out_ref[:, c, first : first + TILE, :] = (one + means[c][None]).astype(
                    jnp.bfloat16
                )


def apply_transform(parts, wide, members, channels, first, block, onto=None):
    slots, count, local_members, rows, lanes = parts[0].shape
    pieces = len(parts)
    strips = slots * pieces // members
    width = members * local_members
    operands = [wide, *parts]
    in_specs = [pl.BlockSpec(wide.shape, lambda i: (0, 0, 0))] + [
        pl.BlockSpec((slots, block, local_members, rows, lanes), lambda i: (0, i, 0, 0, 0))
    ] * pieces
    aliases = {}
    if onto is not None:
        aliases = {len(operands): 0}
        operands.append(onto)
        in_specs.append(pl.BlockSpec(memory_space=pl.ANY))
    skip = first // block
    return pl.pallas_call(
        functools.partial(apply_kernel, members, pieces),
        grid=(count // block,),
        in_specs=in_specs,
        out_specs=pl.BlockSpec(
            (width, block, strips * rows, lanes), lambda i: (0, i + skip, 0, 0)
        ),
        out_shape=jax.ShapeDtypeStruct((width, channels, strips * rows, lanes), jnp.bfloat16),
        input_output_aliases=aliases,
        compiler_params=pltpu.CompilerParams(vmem_limit_bytes=32 << 20),
        cost_estimate=pl.CostEstimate(
            flops=2 * width * count * strips * rows * lanes * width * TILE,
            bytes_accessed=4 * width * count * strips * rows * lanes,
            transcendentals=0,
        ),
    )(*operands)


def apply_plain(recv, late, transform, members):
    slots, _, local_members, rows, lanes = recv.shape
    strips = slots // members
    width = members * local_members
    states = jnp.concatenate([recv, jnp.concatenate(late, axis=0)], axis=1)
    channels = states.shape[1]
    states = states.reshape(members, strips, channels, local_members, rows, lanes)
    mean = jnp.sum(states, axis=(0, 3), dtype=jnp.float32) / width
    pert = (states.astype(jnp.float32) - mean[None, :, :, None]).astype(jnp.bfloat16)
    order = lax.rem(lax.axis_index("member") - jnp.arange(members) + members, members)
    gains = jnp.repeat(transform, BAND, axis=0).reshape(
        strips, rows, members, local_members, width
    )
    gains = jnp.take(gains, order, axis=2)
    gain = jnp.einsum(
        "mjcnxl,jxmnk->kcjxl", pert, gains, preferred_element_type=jnp.float32
    )
    out = mean.transpose(1, 0, 2, 3)[None] + gain
    return out.reshape(width, channels, strips * rows, lanes).astype(jnp.bfloat16)


def local(background, obs_ens, obs_value, obs_precision, obs_row, obs_patch):
    members = lax.axis_size("member")
    regions = lax.axis_size("region")
    obs_rows, width = obs_ens.shape
    capacity = 2 * obs_rows // (members * regions)
    rows = background.shape[2]
    channels = background.shape[1]
    lat_rows = (regions // members) * rows
    filler = jnp.zeros((obs_rows,), jnp.float32)
    columns = [obs_value, obs_precision, obs_row, obs_patch[:, 0]]
    extras = jnp.stack(
        [column.astype(jnp.float32) for column in columns] + [filler] * (EXTRAS - 4)
    )
    recv, late, got = exchange(background, obs_ens.T, extras, capacity)
    for shift in range(1, members):
        ring = [(k, (k + shift) % members) for k in range(members)]
        late[shift] = lax.ppermute(late[shift], "member", ring)
    grams = band_grams(got, width, lat_rows)
    transform = band_transforms(grams, width)
    if rows % TILE:
        return apply_plain(recv, late, transform, members)
    wide = widen(transform, members)
    early = recv.shape[1]
    out = apply_transform([recv], wide, members, channels, 0, math.gcd(early, 2))
    return apply_transform(late, wide, members, channels, early, 1, out)


def solution(mesh):
    in_specs = (
        P("member", None, "region", None),
        P(("member", "region"), None),
        P(("member", "region")),
        P(("member", "region")),
        P(("member", "region")),
        P(("member", "region"), None),
    )
    out_specs = P(None, None, "member", "region")
    return jax.shard_map(local, mesh=mesh, in_specs=in_specs, out_specs=out_specs, check_vma=False)
```

```python
import functools
import math

import jax
import jax.numpy as jnp
from jax import lax
from jax.experimental import pallas as pl
from jax.experimental.pallas import tpu as pltpu
from jax.sharding import PartitionSpec as P


BAND = 2
NS_ITERS = 4
TILE = 8
LANES = 128
LATE = 2
EXTRAS = 8
MESH = pl.DeviceIdType.MESH


def exchange_kernel(
    members, regions, late, bg_ref, ens_ref, value_ref, precision_ref, row_ref, patch_ref, *refs
):
    strips = regions // members
    devices = members * regions
    channels = bg_ref.shape[1]
    recv_ref, own_ref = refs[:2]
    lift_refs = refs[2 : 1 + members]
    got_ref = refs[1 + members]
    (
        held_ref, packed_ref, pair_ref, whole_ref, extra_ref, rank_ref, obs_ref,
        local_sem, spread_send, spread_recv, lift_send, lift_recv, out_sem,
        in_sem, obs_sem,
    ) = refs[2 + members :]
    width, obs_rows = ens_ref.shape
    capacity = obs_ref.shape[2]
    m, r = lax.axis_index("member"), lax.axis_index("region")
    me = m * regions + r
    home, seat = lax.div(r, strips), lax.rem(r, strips)
    first_stage = members * strips
    order = list(range(late, channels)) + list(range(late))

    copies_in = [
        pltpu.make_async_copy(ens_ref, packed_ref.at[0:width], in_sem.at[0]),
        pltpu.make_async_copy(value_ref, pair_ref.at[0], in_sem.at[1]),
        pltpu.make_async_copy(precision_ref, pair_ref.at[1], in_sem.at[2]),
        pltpu.make_async_copy(row_ref, whole_ref.at[0], in_sem.at[3]),
        pltpu.make_async_copy(patch_ref, whole_ref.at[1], in_sem.at[4]),
    ]
    for copy in copies_in:
        copy.start()
    barrier = pltpu.get_barrier_semaphore()

    def at_device(other):
        return {"member": lax.div(other, regions), "region": lax.rem(other, regions)}

    def greet(d, carry):
        other = lax.rem(me + d, devices)
        pl.semaphore_signal(
            barrier, inc=1, device_id=at_device(other), device_id_type=MESH
        )
        return carry

    lax.fori_loop(1, devices, greet, 0)
    pl.semaphore_wait(barrier, devices - 1)

    slot = jnp.where(home == m, seat, first_stage + r)
    groups = [0] + sorted(range(1, members), key=lambda g: (abs(2 * g - members), g))

    def block(c, b):
        return bg_ref.at[:, c, :, pl.ds(pl.multiple_of(b * LANES, LANES), LANES)]

    def spread(c, b):
        pltpu.make_async_remote_copy(
            block(c, b), held_ref.at[slot, c], spread_send.at[c], spread_recv.at[c, home],
            device_id={"region": b}, device_id_type=MESH,
        ).start()

    for c in order:
        pltpu.make_async_copy(block(c, r), held_ref.at[slot, c], local_sem.at[c]).start()
        for j in range(1, strips):
            spread(c, home * strips + lax.rem(seat + j, strips))
        for g in groups[1:]:

            def spread_group(j, carry, c=c, g=g):
                spread(c, lax.rem(home + g, members) * strips + j)
                return carry

            lax.fori_loop(0, strips, spread_group, 0)

    lifted = (members - 1) * strips

    def arrive(c, g):
        a = lax.rem(home + g, members)
        if g == 0:
            pltpu.make_async_copy(held_ref.at[0, c], held_ref.at[0, c], local_sem.at[c]).wait()
        if g or strips > 1:
            some = held_ref.at[0 : strips if g else strips - 1, c]
            pltpu.make_async_copy(some, some, spread_recv.at[c, a]).wait()
        return a

    def forward(c, g):
        a = arrive(c, g)
        s = lax.rem(a - m + members, members)

        @pl.when(a != m)
        def _():
            for j in range(strips):
                pltpu.make_async_remote_copy(
                    held_ref.at[first_stage + a * strips + j, c],
                    held_ref.at[s * strips + j, c],
                    lift_send.at[c], lift_recv.at[c],
                    device_id={"member": a}, device_id_type=MESH,
                ).start()

    early = order[: channels - late]
    ahead = early[: min(3, len(early))]
    for c in ahead:
        forward(c, 0)

    def forward_rest(c):
        for g in groups:
            if g or c not in ahead:
                forward(c, g)

    for copy in copies_in:
        copy.wait()
    obs_lines = obs_rows // LANES
    for k, lines in enumerate([pair_ref[0], pair_ref[1], whole_ref[0], whole_ref[1]]):
        lines = lines.astype(jnp.float32)
        for i in range(obs_lines):
            extra_ref[k : k + 1, i * LANES : (i + 1) * LANES] = lines[i : i + 1]
    extra_ref[4:, :] = jnp.zeros((EXTRAS - 4, obs_rows), jnp.float32)
    packed_ref[width:, :] = extra_ref[...].astype(jnp.bfloat16)
    chunk = math.gcd(obs_rows, 512)
    upper = (
        lax.broadcasted_iota(jnp.int32, (chunk, chunk), 0)
        < lax.broadcasted_iota(jnp.int32, (chunk, chunk), 1)
    ).astype(jnp.bfloat16)
    names = lax.broadcasted_iota(jnp.int32, (devices, 1), 0).astype(jnp.float32)
    offset = jnp.zeros((devices, 1), jnp.float32)
    for k in range(obs_rows // chunk):
        span = slice(k * chunk, (k + 1) * chunk)
        hit = extra_ref[3:4, span] == names
        one = hit.astype(jnp.float32)
        before = offset + jnp.dot(
            one.astype(jnp.bfloat16), upper, preferred_element_type=jnp.float32
        )
        rank_ref[:, span] = jnp.sum(jnp.where(hit, before, 0.0), axis=0, keepdims=True)
        offset = offset + jnp.sum(one, axis=1, keepdims=True)
    places = lax.broadcasted_iota(jnp.int32, (capacity, 1), 0).astype(jnp.float32)

    def place(d, carry):
        total = jnp.zeros((width + EXTRAS, capacity), jnp.float32)
        for k in range(obs_rows // chunk):
            span = slice(k * chunk, (k + 1) * chunk)
            mine = jnp.where(
                extra_ref[3:4, span] == d.astype(jnp.float32), rank_ref[:, span], -1.0
            )
            pick = (places == mine).astype(jnp.float32).astype(jnp.bfloat16)
            total = total + lax.dot_general(
                packed_ref[:, span], pick, (((1,), (1,)), ((), ())),
                preferred_element_type=jnp.float32,
            )
        obs_ref[d] = total.astype(jnp.bfloat16)
        return carry

    stages = min(4, len(early) - 1)
    for k in range(stages):
        forward_rest(early[k])
        lax.fori_loop(devices * k // stages, devices * (k + 1) // stages, place, 0)
    forward_rest(early[stages])

    def send_obs(d, carry):
        other = lax.rem(me + d, devices)
        pltpu.make_async_remote_copy(
            obs_ref.at[other], got_ref.at[me], obs_sem.at[0], obs_sem.at[1],
            device_id=at_device(other), device_id_type=MESH,
        ).start()
        return carry

    lax.fori_loop(1, devices, send_obs, 0)
    pltpu.make_async_copy(obs_ref.at[me], got_ref.at[me], obs_sem.at[2]).start()
    for c in early[stages + 1 :]:
        forward_rest(c)

    def late_copies(c):
        copies = [
            pltpu.make_async_copy(held_ref.at[0:strips, c], own_ref.at[:, c], out_sem.at[c, 0])
        ]
        for s in range(1, members):
            a = lax.rem(m + s, members)
            copies.append(
                pltpu.make_async_copy(
                    held_ref.at[pl.ds(first_stage + a * strips, strips), c],
                    lift_refs[s - 1].at[:, c],
                    out_sem.at[c, s],
                )
            )
        return copies

    for c in range(late):
        for g in groups:
            arrive(c, g)
        for copy in late_copies(c):
            copy.start()

    def early_copy(c):
        return pltpu.make_async_copy(
            held_ref.at[0:first_stage, c], recv_ref.at[:, c - late], out_sem.at[c, 0]
        )

    for c in early:
        lift_all = held_ref.at[0:lifted, c]
        pltpu.make_async_copy(lift_all, lift_all, lift_recv.at[c]).wait()
        early_copy(c).start()
    for c in range(channels):
        spread_all = held_ref.at[0 : regions - 1, c]
        pltpu.make_async_copy(spread_all, spread_all, spread_send.at[c]).wait()
    obs_all = got_ref.at[0 : devices - 1]
    pltpu.make_async_copy(obs_all, obs_all, obs_sem.at[0]).wait()
    pltpu.make_async_copy(obs_all, obs_all, obs_sem.at[1]).wait()
    pltpu.make_async_copy(obs_ref.at[0], got_ref.at[0], obs_sem.at[2]).wait()
    for c in range(late):
        for copy in late_copies(c):
            copy.wait()
    for c in early:
        lift_all = held_ref.at[0:lifted, c]
        pltpu.make_async_copy(lift_all, lift_all, lift_send.at[c]).wait()
        early_copy(c).wait()


def exchange(background, ens_cols, lines, capacity):
    members, regions = lax.axis_size("member"), lax.axis_size("region")
    strips = regions // members
    devices = members * regions
    local_members, channels, rows, _ = background.shape
    width, obs_rows = ens_cols.shape
    obs_lines = obs_rows // LANES
    late = min(LATE, channels - 2)
    dma = pltpu.SemaphoreType.DMA
    kind = background.dtype
    part = jax.ShapeDtypeStruct((strips, late, local_members, rows, LANES), kind)
    out = pl.pallas_call(
        functools.partial(exchange_kernel, members, regions, late),
        in_specs=[pl.BlockSpec(memory_space=pl.ANY)] * 6,
        out_specs=[pl.BlockSpec(memory_space=pl.ANY)] * (members + 2),
        out_shape=[
            jax.ShapeDtypeStruct(
                (members * strips, channels - late, local_members, rows, LANES), kind
            )
        ]
        + [part] * members
        + [jax.ShapeDtypeStruct((devices, width + EXTRAS, capacity), jnp.bfloat16)],
        scratch_shapes=[
            pltpu.VMEM(
                (members * strips + regions, channels, local_members, rows, LANES), kind
            ),
            pltpu.VMEM((width + EXTRAS, obs_rows), jnp.bfloat16),
            pltpu.VMEM((2, obs_lines, LANES), jnp.bfloat16),
            pltpu.VMEM((2, obs_lines, LANES), jnp.int32),
            pltpu.VMEM((EXTRAS, obs_rows), jnp.float32),
            pltpu.VMEM((1, obs_rows), jnp.float32),
            pltpu.VMEM((devices, width + EXTRAS, capacity), jnp.bfloat16),
        ]
        + [dma((channels,))] * 2
        + [dma((channels, members))]
        + [dma((channels,))] * 2
        + [dma((channels, members)), dma((5,)), dma((3,))],
        compiler_params=pltpu.CompilerParams(
            collective_id=0, has_side_effects=True, vmem_limit_bytes=60 << 20
        ),
        cost_estimate=pl.CostEstimate(
            flops=1 << 34, bytes_accessed=4 * background.size, transcendentals=0
        ),
    )(background, ens_cols, *lines)
    return out[0], list(out[1 : 1 + members]), out[1 + members]


def gram_kernel(width, lat_rows, got_ref, gram_ref, proj_ref, scaled_ref):
    bands = lat_rows // BAND

    @pl.when(pl.program_id(0) == 0)
    def _():
        gram_ref[...] = jnp.zeros_like(gram_ref)
        proj_ref[...] = jnp.zeros_like(proj_ref)

    cols = jnp.concatenate(
        [got_ref[k].astype(jnp.float32) for k in range(got_ref.shape[0])], axis=1
    )
    ens = cols[:width]
    obs_val, obs_prec, row = (cols[width + k : width + k + 1] for k in range(3))
    mean = jnp.sum(ens, axis=0, keepdims=True) / width
    pert = (ens - mean).astype(jnp.bfloat16)
    pert_float = pert.astype(jnp.float32)
    innovation = obs_val - mean
    index = lax.broadcasted_iota(jnp.int32, (bands, 1), 0).astype(jnp.float32)
    distance = (row - (index * BAND + (BAND - 1) / 2.0)) / (lat_rows / 4.0)
    weight = obs_prec * jnp.exp(-0.5 * distance * distance)
    for j in range(bands):
        scaled_ref[j * width : (j + 1) * width, :] = (weight[j : j + 1] * pert_float).astype(
            jnp.bfloat16
        )
    over_obs = (((1,), (1,)), ((), ()))
    gram_ref[...] += lax.dot_general(
        scaled_ref[...], pert, over_obs, preferred_element_type=jnp.float32
    )
    proj_ref[...] += lax.dot_general(
        weight * innovation,
        pert_float,
        over_obs,
        precision=lax.Precision.HIGHEST,
        preferred_element_type=jnp.float32,
    )


def band_grams(got, width, lat_rows):
    devices, cols, capacity = got.shape
    bands = lat_rows // BAND
    group = max(1, math.gcd(devices, 1024 // capacity))
    gram, projected = pl.pallas_call(
        functools.partial(gram_kernel, width, lat_rows),
        grid=(devices // group,),
        in_specs=[pl.BlockSpec((group, cols, capacity), lambda i: (i, 0, 0))],
        out_specs=[
            pl.BlockSpec((bands * width, width), lambda i: (0, 0)),
            pl.BlockSpec((bands, width), lambda i: (0, 0)),
        ],
        out_shape=[
            jax.ShapeDtypeStruct((bands * width, width), jnp.float32),
            jax.ShapeDtypeStruct((bands, width), jnp.float32),
        ],
        scratch_shapes=[pltpu.VMEM((bands * width, group * capacity), jnp.bfloat16)],
        compiler_params=pltpu.CompilerParams(vmem_limit_bytes=24 << 20),
        cost_estimate=pl.CostEstimate(
            flops=8 * devices * capacity * bands * width * width,
            bytes_accessed=2 * devices * capacity * cols,
            transcendentals=devices * capacity * bands,
        ),
    )(got)
    return gram.reshape(bands, width, width), projected


def batched(left, right):
    return jnp.einsum("bij,bjk->bik", left, right, precision=lax.Precision.HIGHEST)


def band_transforms(grams, members):
    gram_band, projected = grams
    identity = jnp.eye(members, dtype=jnp.float32)
    system = (members - 1.0) * identity + gram_band
    norm_f = jnp.sqrt(jnp.sum(system * system, axis=(1, 2)))
    root_iter = system / norm_f[:, None, None]
    inv_root = jnp.broadcast_to(identity, system.shape)
    for _ in range(NS_ITERS):
        middle = 1.5 * identity - 0.5 * batched(inv_root, root_iter)
        root_iter = batched(root_iter, middle)
        inv_root = batched(middle, inv_root)
    spread = jnp.sqrt((members - 1.0) / norm_f)[:, None, None] * inv_root
    inverse = batched(inv_root, inv_root) / norm_f[:, None, None]
    mean_shift = jnp.einsum("bjk,bk->bj", inverse, projected, precision=lax.Precision.HIGHEST)
    return (spread + mean_shift[:, :, None]).astype(jnp.bfloat16)


def widen_kernel(transform_ref, wide_ref, turned_ref):
    bands, members, _, width = transform_ref.shape
    side = width * TILE
    m = lax.axis_index("member")
    for s in range(members):
        turned_ref[:, s] = transform_ref[:, lax.rem(m - s + members, members)]
    long = lax.broadcasted_iota(jnp.int32, (side, width), 0)
    repeat = (long // TILE == lax.broadcasted_iota(jnp.int32, (side, width), 1)).astype(
        jnp.bfloat16
    )
    row = lax.broadcasted_iota(jnp.int32, (side, side), 0) % TILE
    col = lax.broadcasted_iota(jnp.int32, (side, side), 1) % TILE
    same = row == col
    over_last = (((1,), (1,)), ((), ()))
    for t in range(bands * BAND // TILE):
        picked = jnp.zeros((side, width), jnp.float32)
        for j in range(TILE // BAND):
            band = turned_ref[t * (TILE // BAND) + j].reshape(width, width)
            tall = lax.dot_general(repeat, band, over_last, preferred_element_type=jnp.float32)
            picked = jnp.where(long % TILE // BAND == j, tall, picked)
        spread = lax.dot_general(
            picked.astype(jnp.bfloat16), repeat, over_last, preferred_element_type=jnp.float32
        )
        wide_ref[t] = jnp.where(same, spread, 0.0).astype(jnp.bfloat16)


def widen(transform, members):
    bands, width, _ = transform.shape
    side = width * TILE
    return pl.pallas_call(
        widen_kernel,
        in_specs=[pl.BlockSpec(memory_space=pltpu.VMEM)],
        out_specs=pl.BlockSpec(memory_space=pltpu.VMEM),
        out_shape=jax.ShapeDtypeStruct((bands * BAND // TILE, side, side), jnp.bfloat16),
        scratch_shapes=[pltpu.VMEM((bands, members, width // members, width), jnp.bfloat16)],
        compiler_params=pltpu.CompilerParams(vmem_limit_bytes=24 << 20),
        cost_estimate=pl.CostEstimate(
            flops=1 << 31, bytes_accessed=8 * side * side, transcendentals=0
        ),
    )(transform.reshape(bands, members, width // members, width))


def tile_gain(parts, wide_ref, members, j, t, block):
    slots, _, local_members, rows, lanes = parts[0].shape
    strips = slots * len(parts) // members
    width = members * local_members
    means, perts = [], []
    for c in range(block):
        states = []
        for s in range(members):
            place = s * strips + j
            states.append(
                parts[place // slots][
                    place % slots, c, :, t * TILE : (t + 1) * TILE, :
                ].astype(jnp.float32)
            )
        state = jnp.concatenate(states, axis=0)
        mean = jnp.sum(state, axis=0) / width
        means.append(mean)
        perts.append((state - mean[None]).reshape(width * TILE, lanes).astype(jnp.bfloat16))
    gain = jnp.dot(
        wide_ref[j * (rows // TILE) + t],
        jnp.concatenate(perts, axis=1),
        preferred_element_type=jnp.float32,
    )
    return [
        (
            gain[:, c * lanes : (c + 1) * lanes].reshape(width, TILE, lanes) + means[c][None]
        ).astype(jnp.bfloat16)
        for c in range(block)
    ]


def apply_kernel(members, wide_ref, part_ref, out_ref):
    slots, block, _, rows, _ = part_ref.shape
    for j in range(slots // members):
        for t in range(rows // TILE):
            first = j * rows + t * TILE
            for c, value in enumerate(tile_gain([part_ref], wide_ref, members, j, t, block)):
                out_ref[:, c, first : first + TILE, :] = value


def apply_early(part, wide, members, channels, block):
    slots, count, local_members, rows, lanes = part.shape
    strips = slots // members
    width = members * local_members
    skip = (channels - count) // block
    return pl.pallas_call(
        functools.partial(apply_kernel, members),
        grid=(pl.cdiv(count, block),),
        in_specs=[
            pl.BlockSpec(wide.shape, lambda i: (0, 0, 0)),
            pl.BlockSpec((slots, block, local_members, rows, lanes), lambda i: (0, i, 0, 0, 0)),
        ],
        out_specs=pl.BlockSpec(
            (width, block, strips * rows, lanes), lambda i: (0, i + skip, 0, 0)
        ),
        out_shape=jax.ShapeDtypeStruct((width, channels, strips * rows, lanes), jnp.bfloat16),
        compiler_params=pltpu.CompilerParams(vmem_limit_bytes=32 << 20),
        cost_estimate=pl.CostEstimate(
            flops=2 * width * count * strips * rows * lanes * width * TILE,
            bytes_accessed=4 * width * count * strips * rows * lanes,
            transcendentals=0,
        ),
    )(wide, part)


def late_kernel(members, wide_ref, *refs):
    parts, (out_ref, done_ref, sem) = refs[:members], refs[members + 1 :]
    strips, block, _, rows, _ = parts[0].shape
    copies = []
    for j in range(strips):
        for t in range(rows // TILE):
            k = j * (rows // TILE) + t
            for c, value in enumerate(tile_gain(parts, wide_ref, members, j, t, block)):
                done_ref[k, :, c] = value
            copy = pltpu.make_async_copy(
                done_ref.at[k],
                out_ref.at[:, 0:block, pl.ds(j * rows + t * TILE, TILE), :],
                sem.at[k],
            )
            copy.start()
            copies.append(copy)
    for copy in copies:
        copy.wait()


def apply_late(parts, wide, members, onto):
    strips, block, local_members, rows, lanes = parts[0].shape
    width = members * local_members
    tiles = strips * rows // TILE
    return pl.pallas_call(
        functools.partial(late_kernel, members),
        in_specs=[pl.BlockSpec(memory_space=pltpu.VMEM)] * (1 + members)
        + [pl.BlockSpec(memory_space=pl.ANY)],
        out_specs=pl.BlockSpec(memory_space=pl.ANY),
        out_shape=jax.ShapeDtypeStruct(onto.shape, onto.dtype),
        input_output_aliases={1 + members: 0},
        scratch_shapes=[
            pltpu.VMEM((tiles, width, block, TILE, lanes), jnp.bfloat16),
            pltpu.SemaphoreType.DMA((tiles,)),
        ],
        compiler_params=pltpu.CompilerParams(vmem_limit_bytes=32 << 20),
        cost_estimate=pl.CostEstimate(
            flops=2 * width * block * strips * rows * lanes * width * TILE,
            bytes_accessed=4 * width * block * strips * rows * lanes,
            transcendentals=0,
        ),
    )(wide, *parts, onto)


def apply_plain(recv, late, transform, members):
    slots, _, local_members, rows, lanes = recv.shape
    strips = slots // members
    width = members * local_members
    states = jnp.concatenate([jnp.concatenate(late, axis=0), recv], axis=1)
    channels = states.shape[1]
    states = states.reshape(members, strips, channels, local_members, rows, lanes)
    mean = jnp.sum(states, axis=(0, 3), dtype=jnp.float32) / width
    pert = (states.astype(jnp.float32) - mean[None, :, :, None]).astype(jnp.bfloat16)
    order = lax.rem(lax.axis_index("member") - jnp.arange(members) + members, members)
    gains = jnp.repeat(transform, BAND, axis=0).reshape(
        strips, rows, members, local_members, width
    )
    gains = jnp.take(gains, order, axis=2)
    gain = jnp.einsum(
        "mjcnxl,jxmnk->kcjxl", pert, gains, preferred_element_type=jnp.float32
    )
    out = mean.transpose(1, 0, 2, 3)[None] + gain
    return out.reshape(width, channels, strips * rows, lanes).astype(jnp.bfloat16)


def local(background, obs_ens, obs_value, obs_precision, obs_row, obs_patch):
    members = lax.axis_size("member")
    regions = lax.axis_size("region")
    obs_rows, width = obs_ens.shape
    capacity = 2 * obs_rows // (members * regions)
    rows = background.shape[2]
    channels = background.shape[1]
    lat_rows = (regions // members) * rows
    lines = [
        column.reshape(obs_rows // LANES, LANES)
        for column in (obs_value, obs_precision, obs_row, obs_patch[:, 0])
    ]
    recv, late, got = exchange(background, obs_ens.T, lines, capacity)
    for shift in range(1, members):
        ring = [(k, (k + shift) % members) for k in range(members)]
        late[shift] = lax.ppermute(late[shift], "member", ring)
    grams = band_grams(got, width, lat_rows)
    transform = band_transforms(grams, width)
    if rows % TILE:
        return apply_plain(recv, late, transform, members)
    wide = widen(transform, members)
    out = apply_early(recv, wide, members, channels, late[0].shape[1])
    return apply_late(late, wide, members, out)


def solution(mesh):
    in_specs = (
        P("member", None, "region", None),
        P(("member", "region"), None),
        P(("member", "region")),
        P(("member", "region")),
        P(("member", "region")),
        P(("member", "region"), None),
    )
    out_specs = P(None, None, "member", "region")
    return jax.shard_map(local, mesh=mesh, in_specs=in_specs, out_specs=out_specs, check_vma=False)
```

```python
import functools
import math

import jax
import jax.numpy as jnp
from jax import lax
from jax.experimental import pallas as pl
from jax.experimental.pallas import tpu as pltpu
from jax.sharding import PartitionSpec as P


BAND = 2
NS_ITERS = 4
TILE = 8
LANES = 128
LATE = 2
EXTRAS = 8
MESH = pl.DeviceIdType.MESH


def add_gram(got_ref, kind, lat_rows, sum_ref, scaled_ref):
    sources, cols, capacity = got_ref.shape[1:]
    width = cols - EXTRAS
    bands = lat_rows // BAND
    lower = bands * width // 2
    group = max(1, math.gcd(sources, 1024 // capacity))
    sum_ref[...] = jnp.zeros_like(sum_ref)

    def step(i, carry):
        block = jnp.concatenate(
            [got_ref[kind, i * group + k].astype(jnp.float32) for k in range(group)], axis=1
        )
        ens = block[:width]
        obs_val, obs_prec, row = (block[width + k : width + k + 1] for k in range(3))
        mean = jnp.sum(ens, axis=0, keepdims=True) / width
        pert = (ens - mean).astype(jnp.bfloat16)
        pert_float = pert.astype(jnp.float32)
        innovation = obs_val - mean
        index = lax.broadcasted_iota(jnp.int32, (bands, 1), 0).astype(jnp.float32)
        distance = (row - (index * BAND + (BAND - 1) / 2.0)) / (lat_rows / 4.0)
        weight = obs_prec * jnp.exp(-0.5 * distance * distance)
        for j in range(bands):
            scaled_ref[j * width : (j + 1) * width, :] = (
                weight[j : j + 1] * pert_float
            ).astype(jnp.bfloat16)
        empty = jnp.zeros_like(pert)
        over_obs = (((1,), (1,)), ((), ()))
        sum_ref[:lower] += lax.dot_general(
            scaled_ref[:lower], jnp.concatenate([pert, empty], axis=0), over_obs,
            preferred_element_type=jnp.float32,
        ) + lax.dot_general(
            scaled_ref[lower:], jnp.concatenate([empty, pert], axis=0), over_obs,
            preferred_element_type=jnp.float32,
        )
        sum_ref[lower:] += lax.dot_general(
            weight * innovation,
            jnp.concatenate([pert_float, jnp.zeros_like(pert_float)], axis=0),
            over_obs,
            precision=lax.Precision.HIGHEST,
            preferred_element_type=jnp.float32,
        )
        return carry

    lax.fori_loop(0, sources // group, step, 0)


def exchange_kernel(
    members, regions, late, bg_ref, ens_ref, value_ref, precision_ref, row_ref, patch_ref, *refs
):
    strips = regions // members
    half = members // 2
    devices = members * regions
    sources = half * regions
    local_members, channels, rows, _ = bg_ref.shape
    recv_ref, own_ref = refs[:2]
    lift_refs = refs[2 : 1 + members]
    near_ref, far_ref = refs[1 + members : 3 + members]
    (
        held_ref, packed_ref, pair_ref, whole_ref, extra_ref, rank_ref, obs_ref, got_ref,
        sum_ref, scaled_ref,
        local_sem, spread_send, spread_recv, lift_send, lift_recv, out_sem,
        in_sem, obs_sem, gram_sem,
    ) = refs[3 + members :]
    width, obs_rows = ens_ref.shape
    capacity = obs_ref.shape[2]
    m, r = lax.axis_index("member"), lax.axis_index("region")
    home, seat = lax.div(r, strips), lax.rem(r, strips)
    side, level = lax.div(m, half), lax.rem(m, half)
    first_stage = members * strips
    order = list(range(late, channels)) + list(range(late))
    early = order[: channels - late]
    pieces = math.gcd(local_members, 4)
    cut = local_members // pieces
    units = [(order[0], k * cut, (k + 1) * cut) for k in range(pieces)]
    units += [(c, 0, local_members) for c in order[1:]]

    copies_in = [
        pltpu.make_async_copy(ens_ref, packed_ref.at[0:width], in_sem.at[0]),
        pltpu.make_async_copy(value_ref, pair_ref.at[0], in_sem.at[1]),
        pltpu.make_async_copy(precision_ref, pair_ref.at[1], in_sem.at[2]),
        pltpu.make_async_copy(row_ref, whole_ref.at[0], in_sem.at[3]),
        pltpu.make_async_copy(patch_ref, whole_ref.at[1], in_sem.at[4]),
    ]
    barrier = pltpu.get_barrier_semaphore()
    for d in range(1, members):
        pl.semaphore_signal(
            barrier, inc=1, device_id={"member": lax.rem(m + d, members)}, device_id_type=MESH
        )

    def greet(d, carry):
        pl.semaphore_signal(
            barrier, inc=1, device_id={"region": lax.rem(r + d, regions)}, device_id_type=MESH
        )
        return carry

    lax.fori_loop(1, regions, greet, 0)
    for copy in copies_in:
        copy.start()
    slot = jnp.where(home == m, seat, first_stage + r)
    groups = [0] + sorted(range(1, members), key=lambda g: (abs(2 * g - members), g))

    def block(u, b):
        c, low, high = units[u]
        return bg_ref.at[low:high, c, :, pl.ds(pl.multiple_of(b * LANES, LANES), LANES)]

    def place_of(u, where):
        c, low, high = units[u]
        return held_ref.at[where, c, low:high]

    def own_copy(u):
        return pltpu.make_async_copy(block(u, r), place_of(u, slot), local_sem.at[u])

    def spread(u, b):
        pltpu.make_async_remote_copy(
            block(u, b), place_of(u, slot), spread_send.at[units[u][0]],
            spread_recv.at[u, home],
            device_id={"region": b}, device_id_type=MESH,
        ).start()

    def issue(u):
        if u >= len(units):
            return
        if u:
            own_copy(u).start()
        for j in range(1, strips):
            spread(u, home * strips + lax.rem(seat + j, strips))
        for g in groups[1:]:

            def spread_group(j, carry, g=g):
                spread(u, lax.rem(home + g, members) * strips + j)
                return carry

            lax.fori_loop(0, strips, spread_group, 0)

    own_copy(0).start()
    pl.semaphore_wait(barrier, regions + members - 2)

    lifted = (members - 1) * strips

    def arrive(u, g):
        c, low, high = units[u]
        a = lax.rem(home + g, members)
        if g == 0:
            own_copy(u).wait()
        if g or strips > 1:
            some = held_ref.at[0 : strips if g else strips - 1, c, low:high]
            pltpu.make_async_copy(some, some, spread_recv.at[u, a]).wait()
        return a

    def forward(u, g):
        c = units[u][0]
        a = arrive(u, g)
        s = lax.rem(a - m + members, members)

        @pl.when(a != m)
        def _():
            for j in range(strips):
                pltpu.make_async_remote_copy(
                    place_of(u, first_stage + a * strips + j),
                    place_of(u, s * strips + j),
                    lift_send.at[c], lift_recv.at[c],
                    device_id={"member": a}, device_id_type=MESH,
                ).start()

    window = pieces + 2
    for u in range(pieces):
        issue(u)
        forward(u, 0)
    for u in range(pieces, window):
        issue(u)
    for g in groups[1:]:
        for u in range(pieces):
            forward(u, g)

    def forward_all(u):
        for g in groups:
            forward(u, g)
        issue(u + 2)

    for copy in copies_in:
        copy.wait()
    obs_lines = obs_rows // LANES
    for k, lines in enumerate([pair_ref[0], pair_ref[1], whole_ref[0], whole_ref[1]]):
        lines = lines.astype(jnp.float32)
        for i in range(obs_lines):
            extra_ref[k : k + 1, i * LANES : (i + 1) * LANES] = lines[i : i + 1]
    extra_ref[4:, :] = jnp.zeros((EXTRAS - 4, obs_rows), jnp.float32)
    packed_ref[width:, :] = extra_ref[...].astype(jnp.bfloat16)
    chunk = math.gcd(obs_rows, 512)
    upper = (
        lax.broadcasted_iota(jnp.int32, (chunk, chunk), 0)
        < lax.broadcasted_iota(jnp.int32, (chunk, chunk), 1)
    ).astype(jnp.bfloat16)
    names = lax.broadcasted_iota(jnp.int32, (devices, 1), 0).astype(jnp.float32)
    offset = jnp.zeros((devices, 1), jnp.float32)
    for k in range(obs_rows // chunk):
        span = slice(k * chunk, (k + 1) * chunk)
        hit = extra_ref[3:4, span] == names
        one = hit.astype(jnp.float32)
        before = offset + jnp.dot(
            one.astype(jnp.bfloat16), upper, preferred_element_type=jnp.float32
        )
        rank_ref[:, span] = jnp.sum(jnp.where(hit, before, 0.0), axis=0, keepdims=True)
        offset = offset + jnp.sum(one, axis=1, keepdims=True)
    places = lax.broadcasted_iota(jnp.int32, (capacity, 1), 0).astype(jnp.float32)

    def place(d, carry):
        total = jnp.zeros((width + EXTRAS, capacity), jnp.float32)
        for k in range(obs_rows // chunk):
            span = slice(k * chunk, (k + 1) * chunk)
            mine = jnp.where(
                extra_ref[3:4, span] == d.astype(jnp.float32), rank_ref[:, span], -1.0
            )
            pick = (places == mine).astype(jnp.float32).astype(jnp.bfloat16)
            total = total + lax.dot_general(
                packed_ref[:, span], pick, (((1,), (1,)), ((), ())),
                preferred_element_type=jnp.float32,
            )
        obs_ref[d] = total.astype(jnp.bfloat16)
        return carry

    rest = list(range(pieces, pieces + len(early) - 1))
    stages = min(4, len(rest) - 1)
    for k in range(stages):
        lax.fori_loop(devices * k // stages, devices * (k + 1) // stages, place, 0)
        forward_all(rest[k])

    def early_copy(c):
        return pltpu.make_async_copy(
            held_ref.at[0:first_stage, c], recv_ref.at[:, c - late], out_sem.at[c, 0]
        )

    def lift_done(c):
        lift_all = held_ref.at[0:lifted, c]
        pltpu.make_async_copy(lift_all, lift_all, lift_recv.at[c]).wait()
        early_copy(c).start()

    lift_done(early[0])
    mine = level * regions + r

    def send_obs(i, carry):
        to = lax.rem(mine + i, sources)
        where = {
            "member": side * half + lax.div(to, regions),
            "region": lax.rem(to, regions),
        }
        for kind in range(2):
            half_of = lax.rem(side + kind, 2)
            pltpu.make_async_remote_copy(
                obs_ref.at[half_of * sources + to], got_ref.at[kind, mine],
                obs_sem.at[kind], obs_sem.at[2 + kind],
                device_id=where, device_id_type=MESH,
            ).start()
        return carry

    lax.fori_loop(1, sources, send_obs, 0)
    for kind in range(2):
        got_ref[kind, mine] = obs_ref[lax.rem(side + kind, 2) * sources + mine]
    for u in rest[stages:]:
        forward_all(u)
    for u in range(rest[-1] + 3, len(units)):
        issue(u)

    def obs_all(kind, sem):
        some = got_ref.at[kind, 0 : sources - 1]
        pltpu.make_async_copy(some, some, obs_sem.at[sem]).wait()

    lat_rows = strips * rows
    for kind in (1, 0):
        obs_all(kind, 2 + kind)
        add_gram(got_ref, kind, lat_rows, sum_ref.at[kind], scaled_ref)
    far = pltpu.make_async_remote_copy(
        sum_ref.at[1], far_ref, gram_sem.at[0], gram_sem.at[1],
        device_id={"member": lax.rem(m + half, members)}, device_id_type=MESH,
    )
    far.start()
    near = pltpu.make_async_copy(sum_ref.at[0], near_ref, gram_sem.at[2])
    near.start()

    def late_copies(c):
        copies = [
            pltpu.make_async_copy(held_ref.at[0:strips, c], own_ref.at[:, c], out_sem.at[c, 0])
        ]
        for s in range(1, members):
            a = lax.rem(m + s, members)
            copies.append(
                pltpu.make_async_copy(
                    held_ref.at[pl.ds(first_stage + a * strips, strips), c],
                    lift_refs[s - 1].at[:, c],
                    out_sem.at[c, s],
                )
            )
        return copies

    for u in range(len(units) - late, len(units)):
        for g in groups:
            arrive(u, g)
        for copy in late_copies(units[u][0]):
            copy.start()
    for c in early[1:]:
        lift_done(c)
    for c in range(channels):
        spread_all = held_ref.at[0 : regions - 1, c]
        pltpu.make_async_copy(spread_all, spread_all, spread_send.at[c]).wait()
    for kind in range(2):
        obs_all(kind, kind)
    for c in range(late):
        for copy in late_copies(c):
            copy.wait()
    for c in early:
        lift_all = held_ref.at[0:lifted, c]
        pltpu.make_async_copy(lift_all, lift_all, lift_send.at[c]).wait()
        early_copy(c).wait()
    near.wait()
    far.wait()


def exchange(background, ens_cols, lines, capacity):
    members, regions = lax.axis_size("member"), lax.axis_size("region")
    strips = regions // members
    devices = members * regions
    sources = devices // 2
    local_members, channels, rows, _ = background.shape
    width, obs_rows = ens_cols.shape
    obs_lines = obs_rows // LANES
    late = min(LATE, channels - 2)
    bands = strips * rows // BAND
    units = channels - 1 + math.gcd(local_members, 4)
    group = max(1, math.gcd(sources, 1024 // capacity))
    dma = pltpu.SemaphoreType.DMA
    kind = background.dtype
    part = jax.ShapeDtypeStruct((strips, late, local_members, rows, LANES), kind)
    total = (bands * width // 2 + bands, 2 * width)
    out = pl.pallas_call(
        functools.partial(exchange_kernel, members, regions, late),
        in_specs=[pl.BlockSpec(memory_space=pl.ANY)] * 6,
        out_specs=[pl.BlockSpec(memory_space=pl.ANY)] * (members + 3),
        out_shape=[
            jax.ShapeDtypeStruct(
                (members * strips, channels - late, local_members, rows, LANES), kind
            )
        ]
        + [part] * members
        + [jax.ShapeDtypeStruct(total, jnp.float32)] * 2,
        scratch_shapes=[
            pltpu.VMEM(
                (members * strips + regions, channels, local_members, rows, LANES), kind
            ),
            pltpu.VMEM((width + EXTRAS, obs_rows), jnp.bfloat16),
            pltpu.VMEM((2, obs_lines, LANES), jnp.bfloat16),
            pltpu.VMEM((2, obs_lines, LANES), jnp.int32),
            pltpu.VMEM((EXTRAS, obs_rows), jnp.float32),
            pltpu.VMEM((1, obs_rows), jnp.float32),
            pltpu.VMEM((devices, width + EXTRAS, capacity), jnp.bfloat16),
            pltpu.VMEM((2, sources, width + EXTRAS, capacity), jnp.bfloat16),
            pltpu.VMEM((2,) + total, jnp.float32),
            pltpu.VMEM((bands * width, group * capacity), jnp.bfloat16),
        ]
        + [dma((units,)), dma((channels,)), dma((units, members))]
        + [dma((channels,))] * 2
        + [dma((channels, members)), dma((5,)), dma((4,)), dma((3,))],
        compiler_params=pltpu.CompilerParams(
            collective_id=0, has_side_effects=True, vmem_limit_bytes=60 << 20
        ),
        cost_estimate=pl.CostEstimate(
            flops=1 << 34, bytes_accessed=4 * background.size, transcendentals=0
        ),
    )(background, ens_cols, *lines)
    return out[0], list(out[1 : 1 + members]), out[1 + members], out[2 + members]


def total_grams(near, far, bands):
    width = near.shape[1] // 2
    total = near + far
    lower = bands * width // 2
    gram = jnp.concatenate(
        [
            total[:lower, :width].reshape(bands // 2, width, width),
            total[:lower, width:].reshape(bands // 2, width, width),
        ]
    )
    return gram, total[lower:, :width]


def batched(left, right):
    return jnp.einsum("bij,bjk->bik", left, right, precision=lax.Precision.HIGHEST)


def band_transforms(grams, members):
    gram_band, projected = grams
    identity = jnp.eye(members, dtype=jnp.float32)
    system = (members - 1.0) * identity + gram_band
    norm_f = jnp.sqrt(jnp.sum(system * system, axis=(1, 2)))
    root_iter = system / norm_f[:, None, None]
    middle = 1.5 * identity - 0.5 * root_iter
    root_iter = batched(root_iter, middle)
    inv_root = middle
    for _ in range(1, NS_ITERS):
        middle = 1.5 * identity - 0.5 * batched(inv_root, root_iter)
        root_iter = batched(root_iter, middle)
        inv_root = batched(middle, inv_root)
    spread = jnp.sqrt((members - 1.0) / norm_f)[:, None, None] * inv_root
    inverse = batched(inv_root, inv_root) / norm_f[:, None, None]
    mean_shift = jnp.einsum("bjk,bk->bj", inverse, projected, precision=lax.Precision.HIGHEST)
    return (spread + mean_shift[:, :, None]).astype(jnp.bfloat16)


def widen_kernel(transform_ref, wide_ref, turned_ref):
    bands, members, _, width = transform_ref.shape
    side = width * TILE
    m = lax.axis_index("member")
    for s in range(members):
        turned_ref[:, s] = transform_ref[:, lax.rem(m - s + members, members)]
    long = lax.broadcasted_iota(jnp.int32, (side, width), 0)
    repeat = (long // TILE == lax.broadcasted_iota(jnp.int32, (side, width), 1)).astype(
        jnp.bfloat16
    )
    row = lax.broadcasted_iota(jnp.int32, (side, side), 0) % TILE
    col = lax.broadcasted_iota(jnp.int32, (side, side), 1) % TILE
    same = row == col
    over_last = (((1,), (1,)), ((), ()))
    for t in range(bands * BAND // TILE):
        picked = jnp.zeros((side, width), jnp.float32)
        for j in range(TILE // BAND):
            band = turned_ref[t * (TILE // BAND) + j].reshape(width, width)
            tall = lax.dot_general(repeat, band, over_last, preferred_element_type=jnp.float32)
            picked = jnp.where(long % TILE // BAND == j, tall, picked)
        spread = lax.dot_general(
            picked.astype(jnp.bfloat16), repeat, over_last, preferred_element_type=jnp.float32
        )
        wide_ref[t] = jnp.where(same, spread, 0.0).astype(jnp.bfloat16)


def widen(transform, members):
    bands, width, _ = transform.shape
    side = width * TILE
    return pl.pallas_call(
        widen_kernel,
        in_specs=[pl.BlockSpec(memory_space=pltpu.VMEM)],
        out_specs=pl.BlockSpec(memory_space=pltpu.VMEM),
        out_shape=jax.ShapeDtypeStruct((bands * BAND // TILE, side, side), jnp.bfloat16),
        scratch_shapes=[pltpu.VMEM((bands, members, width // members, width), jnp.bfloat16)],
        compiler_params=pltpu.CompilerParams(vmem_limit_bytes=24 << 20),
        cost_estimate=pl.CostEstimate(
            flops=1 << 31, bytes_accessed=8 * side * side, transcendentals=0
        ),
    )(transform.reshape(bands, members, width // members, width))


def tile_gain(parts, wide_ref, members, j, t, block):
    slots, _, local_members, rows, lanes = parts[0].shape
    strips = slots * len(parts) // members
    width = members * local_members
    means, perts = [], []
    for c in range(block):
        states = []
        for s in range(members):
            place = s * strips + j
            states.append(
                parts[place // slots][
                    place % slots, c, :, t * TILE : (t + 1) * TILE, :
                ].astype(jnp.float32)
            )
        state = jnp.concatenate(states, axis=0)
        mean = jnp.sum(state, axis=0) / width
        means.append(mean)
        perts.append((state - mean[None]).reshape(width * TILE, lanes).astype(jnp.bfloat16))
    gain = jnp.dot(
        wide_ref[j * (rows // TILE) + t],
        jnp.concatenate(perts, axis=1),
        preferred_element_type=jnp.float32,
    )
    return [
        (
            gain[:, c * lanes : (c + 1) * lanes].reshape(width, TILE, lanes) + means[c][None]
        ).astype(jnp.bfloat16)
        for c in range(block)
    ]


def apply_kernel(members, wide_ref, part_ref, out_ref):
    slots, block, _, rows, _ = part_ref.shape
    for j in range(slots // members):
        for t in range(rows // TILE):
            first = j * rows + t * TILE
            for c, value in enumerate(tile_gain([part_ref], wide_ref, members, j, t, block)):
                out_ref[:, c, first : first + TILE, :] = value


def apply_early(part, wide, members, channels, block):
    slots, count, local_members, rows, lanes = part.shape
    strips = slots // members
    width = members * local_members
    skip = (channels - count) // block
    return pl.pallas_call(
        functools.partial(apply_kernel, members),
        grid=(pl.cdiv(count, block),),
        in_specs=[
            pl.BlockSpec(wide.shape, lambda i: (0, 0, 0)),
            pl.BlockSpec((slots, block, local_members, rows, lanes), lambda i: (0, i, 0, 0, 0)),
        ],
        out_specs=pl.BlockSpec(
            (width, block, strips * rows, lanes), lambda i: (0, i + skip, 0, 0)
        ),
        out_shape=jax.ShapeDtypeStruct((width, channels, strips * rows, lanes), jnp.bfloat16),
        compiler_params=pltpu.CompilerParams(vmem_limit_bytes=32 << 20),
        cost_estimate=pl.CostEstimate(
            flops=2 * width * count * strips * rows * lanes * width * TILE,
            bytes_accessed=4 * width * count * strips * rows * lanes,
            transcendentals=0,
        ),
    )(wide, part)


def late_kernel(members, wide_ref, *refs):
    parts, (out_ref, done_ref, sem) = refs[:members], refs[members + 1 :]
    strips, block, _, rows, _ = parts[0].shape
    copies = []
    for j in range(strips):
        for t in range(rows // TILE):
            k = j * (rows // TILE) + t
            for c, value in enumerate(tile_gain(parts, wide_ref, members, j, t, block)):
                done_ref[k, :, c] = value
            copy = pltpu.make_async_copy(
                done_ref.at[k],
                out_ref.at[:, 0:block, pl.ds(j * rows + t * TILE, TILE), :],
                sem.at[k],
            )
            copy.start()
            copies.append(copy)
    for copy in copies:
        copy.wait()


def apply_late(parts, wide, members, onto):
    strips, block, local_members, rows, lanes = parts[0].shape
    width = members * local_members
    tiles = strips * rows // TILE
    return pl.pallas_call(
        functools.partial(late_kernel, members),
        in_specs=[pl.BlockSpec(memory_space=pltpu.VMEM)] * (1 + members)
        + [pl.BlockSpec(memory_space=pl.ANY)],
        out_specs=pl.BlockSpec(memory_space=pl.ANY),
        out_shape=jax.ShapeDtypeStruct(onto.shape, onto.dtype),
        input_output_aliases={1 + members: 0},
        scratch_shapes=[
            pltpu.VMEM((tiles, width, block, TILE, lanes), jnp.bfloat16),
            pltpu.SemaphoreType.DMA((tiles,)),
        ],
        compiler_params=pltpu.CompilerParams(vmem_limit_bytes=32 << 20),
        cost_estimate=pl.CostEstimate(
            flops=2 * width * block * strips * rows * lanes * width * TILE,
            bytes_accessed=4 * width * block * strips * rows * lanes,
            transcendentals=0,
        ),
    )(wide, *parts, onto)


def apply_plain(recv, late, transform, members):
    slots, _, local_members, rows, lanes = recv.shape
    strips = slots // members
    width = members * local_members
    states = jnp.concatenate([jnp.concatenate(late, axis=0), recv], axis=1)
    channels = states.shape[1]
    states = states.reshape(members, strips, channels, local_members, rows, lanes)
    mean = jnp.sum(states, axis=(0, 3), dtype=jnp.float32) / width
    pert = (states.astype(jnp.float32) - mean[None, :, :, None]).astype(jnp.bfloat16)
    order = lax.rem(lax.axis_index("member") - jnp.arange(members) + members, members)
    gains = jnp.repeat(transform, BAND, axis=0).reshape(
        strips, rows, members, local_members, width
    )
    gains = jnp.take(gains, order, axis=2)
    gain = jnp.einsum(
        "mjcnxl,jxmnk->kcjxl", pert, gains, preferred_element_type=jnp.float32
    )
    out = mean.transpose(1, 0, 2, 3)[None] + gain
    return out.reshape(width, channels, strips * rows, lanes).astype(jnp.bfloat16)


def local(background, obs_ens, obs_value, obs_precision, obs_row, obs_patch):
    members = lax.axis_size("member")
    regions = lax.axis_size("region")
    obs_rows, width = obs_ens.shape
    capacity = 2 * obs_rows // (members * regions)
    rows = background.shape[2]
    channels = background.shape[1]
    lat_rows = (regions // members) * rows
    lines = [
        column.reshape(obs_rows // LANES, LANES)
        for column in (obs_value, obs_precision, obs_row, obs_patch[:, 0])
    ]
    recv, late, near, far = exchange(background, obs_ens.T, lines, capacity)
    for shift in range(1, members):
        ring = [(k, (k + shift) % members) for k in range(members)]
        late[shift] = lax.ppermute(late[shift], "member", ring)
    transform = band_transforms(total_grams(near, far, lat_rows // BAND), width)
    if rows % TILE:
        return apply_plain(recv, late, transform, members)
    wide = widen(transform, members)
    out = apply_early(recv, wide, members, channels, late[0].shape[1])
    return apply_late(late, wide, members, out)


def solution(mesh):
    in_specs = (
        P("member", None, "region", None),
        P(("member", "region"), None),
        P(("member", "region")),
        P(("member", "region")),
        P(("member", "region")),
        P(("member", "region"), None),
    )
    out_specs = P(None, None, "member", "region")
    return jax.shard_map(local, mesh=mesh, in_specs=in_specs, out_specs=out_specs, check_vma=False)
```

```python
import functools
import math

import jax
import jax.numpy as jnp
from jax import lax
from jax.experimental import pallas as pl
from jax.experimental.pallas import tpu as pltpu
from jax.sharding import PartitionSpec as P


BAND = 2
NS_ITERS = 4
TILE = 8
LANES = 128
LATE = 3
EXTRAS = 8
MESH = pl.DeviceIdType.MESH


def add_gram(got_ref, kind, lat_rows, sum_ref, scaled_ref):
    sources, cols, capacity = got_ref.shape[1:]
    width = cols - EXTRAS
    bands = lat_rows // BAND
    lower = bands * width // 2
    group = max(1, math.gcd(sources, 1024 // capacity))
    sum_ref[...] = jnp.zeros_like(sum_ref)
    last = lower + bands

    def step(i, carry):
        block = jnp.concatenate(
            [got_ref[kind, i * group + k].astype(jnp.float32) for k in range(group)], axis=1
        )
        ens = block[:width]
        obs_val, obs_prec, row = (block[width + k : width + k + 1] for k in range(3))
        mean = jnp.sum(ens, axis=0, keepdims=True) / width
        pert = (ens - mean).astype(jnp.bfloat16)
        pert_float = pert.astype(jnp.float32)
        innovation = obs_val - mean
        index = lax.broadcasted_iota(jnp.int32, (bands, 1), 0).astype(jnp.float32)
        distance = (row - (index * BAND + (BAND - 1) / 2.0)) / (lat_rows / 4.0)
        weight = obs_prec * jnp.exp(-0.5 * distance * distance)
        for j in range(bands):
            scaled_ref[j * width : (j + 1) * width, :] = (
                weight[j : j + 1] * pert_float
            ).astype(jnp.bfloat16)
        empty = jnp.zeros_like(pert)
        over_obs = (((1,), (1,)), ((), ()))
        sum_ref[:lower] += lax.dot_general(
            scaled_ref[:lower], jnp.concatenate([pert, empty], axis=0), over_obs,
            preferred_element_type=jnp.float32,
        ) + lax.dot_general(
            scaled_ref[lower:], jnp.concatenate([empty, pert], axis=0), over_obs,
            preferred_element_type=jnp.float32,
        )
        sum_ref[lower:last] += lax.dot_general(
            weight * innovation,
            jnp.concatenate([pert_float, jnp.zeros_like(pert_float)], axis=0),
            over_obs,
            precision=lax.Precision.HIGHEST,
            preferred_element_type=jnp.float32,
        )
        return carry

    lax.fori_loop(0, sources // group, step, 0)


def split_gram(sum_ref, sent_ref, bands):
    width = sum_ref.shape[1] // 2
    lower = bands * width // 2
    last = lower + bands
    gram = sum_ref[:lower]
    sent_ref[...] = gram.astype(jnp.bfloat16)
    diagonal = (
        lax.broadcasted_iota(jnp.int32, (width, 2 * width), 0)
        == lax.broadcasted_iota(jnp.int32, (width, 2 * width), 1) % width
    )
    for j in range(bands // 2):
        one = jnp.where(diagonal, gram[j * width : (j + 1) * width], 0.0)
        sum_ref[last + j : last + j + 1] = jnp.sum(one, axis=0, keepdims=True)


def exchange_kernel(
    members, regions, late, bg_ref, ens_ref, value_ref, precision_ref, row_ref, patch_ref, *refs
):
    strips = regions // members
    half = members // 2
    devices = members * regions
    sources = half * regions
    local_members, channels, rows, _ = bg_ref.shape
    recv_ref, own_ref = refs[:2]
    lift_refs = refs[2 : 1 + members]
    near_ref, far_ref, edge_ref = refs[1 + members : 4 + members]
    (
        held_ref, packed_ref, pair_ref, whole_ref, extra_ref, rank_ref, obs_ref, got_ref,
        sum_ref, sent_ref, scaled_ref,
        local_sem, spread_send, spread_recv, lift_send, lift_recv, out_sem,
        in_sem, obs_sem, gram_sem,
    ) = refs[4 + members :]
    width, obs_rows = ens_ref.shape
    capacity = obs_ref.shape[2]
    m, r = lax.axis_index("member"), lax.axis_index("region")
    home, seat = lax.div(r, strips), lax.rem(r, strips)
    side, level = lax.div(m, half), lax.rem(m, half)
    first_stage = members * strips
    order = list(range(channels))
    first_late = channels - late
    early = order[: channels - late]
    pieces = math.gcd(local_members, 4)
    cut = local_members // pieces
    units = [(order[0], k * cut, (k + 1) * cut) for k in range(pieces)]
    units += [(c, 0, local_members) for c in order[1:]]

    copies_in = [
        pltpu.make_async_copy(ens_ref, packed_ref.at[0:width], in_sem.at[0]),
        pltpu.make_async_copy(value_ref, pair_ref.at[0], in_sem.at[1]),
        pltpu.make_async_copy(precision_ref, pair_ref.at[1], in_sem.at[2]),
        pltpu.make_async_copy(row_ref, whole_ref.at[0], in_sem.at[3]),
        pltpu.make_async_copy(patch_ref, whole_ref.at[1], in_sem.at[4]),
    ]
    barrier = pltpu.get_barrier_semaphore()
    for d in range(1, members):
        pl.semaphore_signal(
            barrier, inc=1, device_id={"member": lax.rem(m + d, members)}, device_id_type=MESH
        )

    def greet(d, carry):
        pl.semaphore_signal(
            barrier, inc=1, device_id={"region": lax.rem(r + d, regions)}, device_id_type=MESH
        )
        return carry

    lax.fori_loop(1, regions, greet, 0)
    for copy in copies_in:
        copy.start()
    slot = jnp.where(home == m, seat, first_stage + r)
    groups = [0] + sorted(range(1, members), key=lambda g: (abs(2 * g - members), g))

    def block(u, b):
        c, low, high = units[u]
        return bg_ref.at[low:high, c, :, pl.ds(pl.multiple_of(b * LANES, LANES), LANES)]

    def place_of(u, where):
        c, low, high = units[u]
        return held_ref.at[where, c, low:high]

    def own_copy(u):
        return pltpu.make_async_copy(block(u, r), place_of(u, slot), local_sem.at[u])

    def spread(u, b):
        pltpu.make_async_remote_copy(
            block(u, b), place_of(u, slot), spread_send.at[units[u][0]],
            spread_recv.at[u, home],
            device_id={"region": b}, device_id_type=MESH,
        ).start()

    def issue(u):
        if u >= len(units):
            return
        if u:
            own_copy(u).start()
        for j in range(1, strips):
            spread(u, home * strips + lax.rem(seat + j, strips))
        for g in groups[1:]:

            def spread_group(j, carry, g=g):
                spread(u, lax.rem(home + g, members) * strips + j)
                return carry

            lax.fori_loop(0, strips, spread_group, 0)

    own_copy(0).start()
    pl.semaphore_wait(barrier, regions + members - 2)

    lifted = (members - 1) * strips

    def arrive(u, g):
        c, low, high = units[u]
        a = lax.rem(home + g, members)
        if g == 0:
            own_copy(u).wait()
        if g or strips > 1:
            some = held_ref.at[0 : strips if g else strips - 1, c, low:high]
            pltpu.make_async_copy(some, some, spread_recv.at[u, a]).wait()
        return a

    def forward(u, g):
        c = units[u][0]
        a = arrive(u, g)
        s = lax.rem(a - m + members, members)

        @pl.when(a != m)
        def _():
            for j in range(strips):
                pltpu.make_async_remote_copy(
                    place_of(u, first_stage + a * strips + j),
                    place_of(u, s * strips + j),
                    lift_send.at[c], lift_recv.at[c],
                    device_id={"member": a}, device_id_type=MESH,
                ).start()

    window = pieces + 2
    for u in range(pieces):
        issue(u)
        forward(u, 0)
    for u in range(pieces, window):
        issue(u)
    for g in groups[1:]:
        for u in range(pieces):
            forward(u, g)

    def forward_all(u):
        for g in groups:
            forward(u, g)
        issue(u + 2)

    for copy in copies_in:
        copy.wait()
    obs_lines = obs_rows // LANES
    for k, lines in enumerate([pair_ref[0], pair_ref[1], whole_ref[0], whole_ref[1]]):
        lines = lines.astype(jnp.float32)
        for i in range(obs_lines):
            extra_ref[k : k + 1, i * LANES : (i + 1) * LANES] = lines[i : i + 1]
    extra_ref[4:, :] = jnp.zeros((EXTRAS - 4, obs_rows), jnp.float32)
    packed_ref[width:, :] = extra_ref[...].astype(jnp.bfloat16)
    chunk = math.gcd(obs_rows, 512)
    upper = (
        lax.broadcasted_iota(jnp.int32, (chunk, chunk), 0)
        < lax.broadcasted_iota(jnp.int32, (chunk, chunk), 1)
    ).astype(jnp.bfloat16)
    names = lax.broadcasted_iota(jnp.int32, (devices, 1), 0).astype(jnp.float32)
    offset = jnp.zeros((devices, 1), jnp.float32)
    for k in range(obs_rows // chunk):
        span = slice(k * chunk, (k + 1) * chunk)
        hit = extra_ref[3:4, span] == names
        one = hit.astype(jnp.float32)
        before = offset + jnp.dot(
            one.astype(jnp.bfloat16), upper, preferred_element_type=jnp.float32
        )
        rank_ref[:, span] = jnp.sum(jnp.where(hit, before, 0.0), axis=0, keepdims=True)
        offset = offset + jnp.sum(one, axis=1, keepdims=True)
    places = lax.broadcasted_iota(jnp.int32, (capacity, 1), 0).astype(jnp.float32)

    def place(d, carry):
        total = jnp.zeros((width + EXTRAS, capacity), jnp.float32)
        for k in range(obs_rows // chunk):
            span = slice(k * chunk, (k + 1) * chunk)
            mine = jnp.where(
                extra_ref[3:4, span] == d.astype(jnp.float32), rank_ref[:, span], -1.0
            )
            pick = (places == mine).astype(jnp.float32).astype(jnp.bfloat16)
            total = total + lax.dot_general(
                packed_ref[:, span], pick, (((1,), (1,)), ((), ())),
                preferred_element_type=jnp.float32,
            )
        obs_ref[d] = total.astype(jnp.bfloat16)
        return carry

    rest = list(range(pieces, pieces + len(early) - 1))
    stages = min(4, len(rest) - 1)
    for k in range(stages):
        lax.fori_loop(devices * k // stages, devices * (k + 1) // stages, place, 0)
        forward_all(rest[k])

    def early_copy(c):
        return pltpu.make_async_copy(
            held_ref.at[0:first_stage, c], recv_ref.at[:, c], out_sem.at[c, 0]
        )

    def lift_done(c):
        lift_all = held_ref.at[0:lifted, c]
        pltpu.make_async_copy(lift_all, lift_all, lift_recv.at[c]).wait()
        early_copy(c).start()

    lift_done(early[0])
    mine = level * regions + r

    def send_obs(i, carry):
        to = lax.rem(mine + i, sources)
        where = {
            "member": side * half + lax.div(to, regions),
            "region": lax.rem(to, regions),
        }
        for kind in range(2):
            half_of = lax.rem(side + kind, 2)
            pltpu.make_async_remote_copy(
                obs_ref.at[half_of * sources + to], got_ref.at[kind, mine],
                obs_sem.at[kind], obs_sem.at[2 + kind],
                device_id=where, device_id_type=MESH,
            ).start()
        return carry

    lax.fori_loop(1, sources, send_obs, 0)
    for kind in range(2):
        got_ref[kind, mine] = obs_ref[lax.rem(side + kind, 2) * sources + mine]
    for u in rest[stages:]:
        forward_all(u)
    for u in range(rest[-1] + 3, len(units)):
        issue(u)

    def obs_all(kind, sem):
        some = got_ref.at[kind, 0 : sources - 1]
        pltpu.make_async_copy(some, some, obs_sem.at[sem]).wait()

    lat_rows = strips * rows
    for kind in (1, 0):
        obs_all(kind, 2 + kind)
        add_gram(got_ref, kind, lat_rows, sum_ref.at[kind], scaled_ref)
        if kind:
            split_gram(sum_ref.at[1], sent_ref, lat_rows // BAND)
    lower = sent_ref.shape[0]
    across = {"member": lax.rem(m + half, members)}
    far = [
        pltpu.make_async_remote_copy(
            sent_ref, far_ref, gram_sem.at[0], gram_sem.at[1],
            device_id=across, device_id_type=MESH,
        ),
        pltpu.make_async_remote_copy(
            sum_ref.at[1, lower:], edge_ref, gram_sem.at[2], gram_sem.at[3],
            device_id=across, device_id_type=MESH,
        ),
    ]
    for copy in far:
        copy.start()
    near = pltpu.make_async_copy(sum_ref.at[0], near_ref, gram_sem.at[4])
    near.start()

    def late_copies(c):
        copies = [
            pltpu.make_async_copy(held_ref.at[0:strips, c], own_ref.at[:, c - first_late], out_sem.at[c, 0])
        ]
        for s in range(1, members):
            a = lax.rem(m + s, members)
            copies.append(
                pltpu.make_async_copy(
                    held_ref.at[pl.ds(first_stage + a * strips, strips), c],
                    lift_refs[s - 1].at[:, c - first_late],
                    out_sem.at[c, s],
                )
            )
        return copies

    for u in range(len(units) - late, len(units)):
        for g in groups:
            arrive(u, g)
        for copy in late_copies(units[u][0]):
            copy.start()
    for c in early[1:]:
        lift_done(c)
    for c in range(channels):
        spread_all = held_ref.at[0 : regions - 1, c]
        pltpu.make_async_copy(spread_all, spread_all, spread_send.at[c]).wait()
    for kind in range(2):
        obs_all(kind, kind)
    for c in order[channels - late :]:
        for copy in late_copies(c):
            copy.wait()
    for c in early:
        lift_all = held_ref.at[0:lifted, c]
        pltpu.make_async_copy(lift_all, lift_all, lift_send.at[c]).wait()
        early_copy(c).wait()
    near.wait()
    for copy in far:
        copy.wait()


def exchange(background, ens_cols, lines, capacity):
    members, regions = lax.axis_size("member"), lax.axis_size("region")
    strips = regions // members
    devices = members * regions
    sources = devices // 2
    local_members, channels, rows, _ = background.shape
    width, obs_rows = ens_cols.shape
    obs_lines = obs_rows // LANES
    late = min(LATE, channels - 2)
    bands = strips * rows // BAND
    units = channels - 1 + math.gcd(local_members, 4)
    group = max(1, math.gcd(sources, 1024 // capacity))
    dma = pltpu.SemaphoreType.DMA
    kind = background.dtype
    part = jax.ShapeDtypeStruct((strips, late, local_members, rows, LANES), kind)
    lower = bands * width // 2
    edge = (3 * bands // 2 + 7) // 8 * 8
    total = (lower + edge, 2 * width)
    out = pl.pallas_call(
        functools.partial(exchange_kernel, members, regions, late),
        in_specs=[pl.BlockSpec(memory_space=pl.ANY)] * 6,
        out_specs=[pl.BlockSpec(memory_space=pl.ANY)] * (members + 4),
        out_shape=[
            jax.ShapeDtypeStruct(
                (members * strips, channels - late, local_members, rows, LANES), kind
            )
        ]
        + [part] * members
        + [
            jax.ShapeDtypeStruct(total, jnp.float32),
            jax.ShapeDtypeStruct((lower, 2 * width), jnp.bfloat16),
            jax.ShapeDtypeStruct((edge, 2 * width), jnp.float32),
        ],
        scratch_shapes=[
            pltpu.VMEM(
                (members * strips + regions, channels, local_members, rows, LANES), kind
            ),
            pltpu.VMEM((width + EXTRAS, obs_rows), jnp.bfloat16),
            pltpu.VMEM((2, obs_lines, LANES), jnp.bfloat16),
            pltpu.VMEM((2, obs_lines, LANES), jnp.int32),
            pltpu.VMEM((EXTRAS, obs_rows), jnp.float32),
            pltpu.VMEM((1, obs_rows), jnp.float32),
            pltpu.VMEM((devices, width + EXTRAS, capacity), jnp.bfloat16),
            pltpu.VMEM((2, sources, width + EXTRAS, capacity), jnp.bfloat16),
            pltpu.VMEM((2,) + total, jnp.float32),
            pltpu.VMEM((lower, 2 * width), jnp.bfloat16),
            pltpu.VMEM((bands * width, group * capacity), jnp.bfloat16),
        ]
        + [dma((units,)), dma((channels,)), dma((units, members))]
        + [dma((channels,))] * 2
        + [dma((channels, members)), dma((5,)), dma((4,)), dma((5,))],
        compiler_params=pltpu.CompilerParams(
            collective_id=0, has_side_effects=True, vmem_limit_bytes=60 << 20
        ),
        cost_estimate=pl.CostEstimate(
            flops=1 << 34, bytes_accessed=4 * background.size, transcendentals=0
        ),
    )(background, ens_cols, *lines)
    return out[0], list(out[1 : 1 + members]), out[1 + members :]


def total_grams(sums, bands):
    near, far, edge = sums
    lower, width = far.shape[0], far.shape[1] // 2
    same = (
        lax.broadcasted_iota(jnp.int32, (bands // 2, width, 2 * width), 1)
        == lax.broadcasted_iota(jnp.int32, (bands // 2, width, 2 * width), 2) % width
    )
    diagonal = edge[bands : bands + bands // 2][:, None, :]
    other = far.astype(jnp.float32).reshape(bands // 2, width, 2 * width)
    total = near[:lower].reshape(other.shape) + jnp.where(same, diagonal, other)
    gram = jnp.concatenate([total[:, :, :width], total[:, :, width:]])
    projected = near[lower : lower + bands] + edge[:bands]
    return gram, projected[:, :width]


def batched(left, right):
    return jnp.einsum("bij,bjk->bik", left, right, precision=lax.Precision.HIGHEST)


def band_transforms(grams, members):
    gram_band, projected = grams
    identity = jnp.eye(members, dtype=jnp.float32)
    system = (members - 1.0) * identity + gram_band
    norm_f = jnp.sqrt(jnp.sum(system * system, axis=(1, 2)))
    root_iter = system / norm_f[:, None, None]
    middle = 1.5 * identity - 0.5 * root_iter
    root_iter = batched(root_iter, middle)
    inv_root = middle
    for _ in range(1, NS_ITERS):
        middle = 1.5 * identity - 0.5 * batched(inv_root, root_iter)
        root_iter = batched(root_iter, middle)
        inv_root = batched(middle, inv_root)
    spread = jnp.sqrt((members - 1.0) / norm_f)[:, None, None] * inv_root
    inverse = batched(inv_root, inv_root) / norm_f[:, None, None]
    mean_shift = jnp.einsum("bjk,bk->bj", inverse, projected, precision=lax.Precision.HIGHEST)
    return (spread + mean_shift[:, :, None]).astype(jnp.bfloat16)


def widen_kernel(transform_ref, wide_ref, turned_ref):
    bands, members, _, width = transform_ref.shape
    side = width * TILE
    m = lax.axis_index("member")
    for s in range(members):
        turned_ref[:, s] = transform_ref[:, lax.rem(m - s + members, members)]
    long = lax.broadcasted_iota(jnp.int32, (side, width), 0)
    repeat = (long // TILE == lax.broadcasted_iota(jnp.int32, (side, width), 1)).astype(
        jnp.bfloat16
    )
    row = lax.broadcasted_iota(jnp.int32, (side, side), 0) % TILE
    col = lax.broadcasted_iota(jnp.int32, (side, side), 1) % TILE
    same = row == col
    over_last = (((1,), (1,)), ((), ()))
    for t in range(bands * BAND // TILE):
        picked = jnp.zeros((side, width), jnp.float32)
        for j in range(TILE // BAND):
            band = turned_ref[t * (TILE // BAND) + j].reshape(width, width)
            tall = lax.dot_general(repeat, band, over_last, preferred_element_type=jnp.float32)
            picked = jnp.where(long % TILE // BAND == j, tall, picked)
        spread = lax.dot_general(
            picked.astype(jnp.bfloat16), repeat, over_last, preferred_element_type=jnp.float32
        )
        wide_ref[t] = jnp.where(same, spread, 0.0).astype(jnp.bfloat16)


def widen(transform, members):
    bands, width, _ = transform.shape
    side = width * TILE
    return pl.pallas_call(
        widen_kernel,
        in_specs=[pl.BlockSpec(memory_space=pltpu.VMEM)],
        out_specs=pl.BlockSpec(memory_space=pltpu.VMEM),
        out_shape=jax.ShapeDtypeStruct((bands * BAND // TILE, side, side), jnp.bfloat16),
        scratch_shapes=[pltpu.VMEM((bands, members, width // members, width), jnp.bfloat16)],
        compiler_params=pltpu.CompilerParams(vmem_limit_bytes=24 << 20),
        cost_estimate=pl.CostEstimate(
            flops=1 << 31, bytes_accessed=8 * side * side, transcendentals=0
        ),
    )(transform.reshape(bands, members, width // members, width))


def tile_gain(parts, wide_ref, members, j, t, block):
    slots, _, local_members, rows, lanes = parts[0].shape
    strips = slots * len(parts) // members
    width = members * local_members
    means, perts = [], []
    for c in range(block):
        states = []
        for s in range(members):
            place = s * strips + j
            states.append(
                parts[place // slots][
                    place % slots, c, :, t * TILE : (t + 1) * TILE, :
                ].astype(jnp.float32)
            )
        state = jnp.concatenate(states, axis=0)
        mean = jnp.sum(state, axis=0) / width
        means.append(mean)
        perts.append((state - mean[None]).reshape(width * TILE, lanes).astype(jnp.bfloat16))
    gain = jnp.dot(
        wide_ref[j * (rows // TILE) + t],
        jnp.concatenate(perts, axis=1),
        preferred_element_type=jnp.float32,
    )
    return [
        (
            gain[:, c * lanes : (c + 1) * lanes].reshape(width, TILE, lanes) + means[c][None]
        ).astype(jnp.bfloat16)
        for c in range(block)
    ]


def apply_kernel(members, wide_ref, part_ref, out_ref):
    slots, block, _, rows, _ = part_ref.shape
    for j in range(slots // members):
        for t in range(rows // TILE):
            first = j * rows + t * TILE
            for c, value in enumerate(tile_gain([part_ref], wide_ref, members, j, t, block)):
                out_ref[:, c, first : first + TILE, :] = value


def apply_early(part, wide, members, channels, block):
    slots, count, local_members, rows, lanes = part.shape
    strips = slots // members
    width = members * local_members
    return pl.pallas_call(
        functools.partial(apply_kernel, members),
        grid=(pl.cdiv(count, block),),
        in_specs=[
            pl.BlockSpec(wide.shape, lambda i: (0, 0, 0)),
            pl.BlockSpec((slots, block, local_members, rows, lanes), lambda i: (0, i, 0, 0, 0)),
        ],
        out_specs=pl.BlockSpec(
            (width, block, strips * rows, lanes), lambda i: (0, i, 0, 0)
        ),
        out_shape=jax.ShapeDtypeStruct((width, channels, strips * rows, lanes), jnp.bfloat16),
        compiler_params=pltpu.CompilerParams(vmem_limit_bytes=32 << 20),
        cost_estimate=pl.CostEstimate(
            flops=2 * width * count * strips * rows * lanes * width * TILE,
            bytes_accessed=4 * width * count * strips * rows * lanes,
            transcendentals=0,
        ),
    )(wide, part)


def late_kernel(members, wide_ref, *refs):
    parts, (out_ref, done_ref, sem) = refs[:members], refs[members + 1 :]
    strips, block, _, rows, _ = parts[0].shape
    first = out_ref.shape[1] - block
    copies = []
    for j in range(strips):
        for t in range(rows // TILE):
            k = j * (rows // TILE) + t
            for c, value in enumerate(tile_gain(parts, wide_ref, members, j, t, block)):
                done_ref[k, :, c] = value
            copy = pltpu.make_async_copy(
                done_ref.at[k],
                out_ref.at[:, first : first + block, pl.ds(j * rows + t * TILE, TILE), :],
                sem.at[k],
            )
            copy.start()
            copies.append(copy)
    for copy in copies:
        copy.wait()


def apply_late(parts, wide, members, onto):
    strips, block, local_members, rows, lanes = parts[0].shape
    width = members * local_members
    tiles = strips * rows // TILE
    return pl.pallas_call(
        functools.partial(late_kernel, members),
        in_specs=[pl.BlockSpec(memory_space=pltpu.VMEM)] * (1 + members)
        + [pl.BlockSpec(memory_space=pl.ANY)],
        out_specs=pl.BlockSpec(memory_space=pl.ANY),
        out_shape=jax.ShapeDtypeStruct(onto.shape, onto.dtype),
        input_output_aliases={1 + members: 0},
        scratch_shapes=[
            pltpu.VMEM((tiles, width, block, TILE, lanes), jnp.bfloat16),
            pltpu.SemaphoreType.DMA((tiles,)),
        ],
        compiler_params=pltpu.CompilerParams(vmem_limit_bytes=32 << 20),
        cost_estimate=pl.CostEstimate(
            flops=2 * width * block * strips * rows * lanes * width * TILE,
            bytes_accessed=4 * width * block * strips * rows * lanes,
            transcendentals=0,
        ),
    )(wide, *parts, onto)


def apply_plain(recv, late, transform, members):
    slots, _, local_members, rows, lanes = recv.shape
    strips = slots // members
    width = members * local_members
    states = jnp.concatenate([recv, jnp.concatenate(late, axis=0)], axis=1)
    channels = states.shape[1]
    states = states.reshape(members, strips, channels, local_members, rows, lanes)
    mean = jnp.sum(states, axis=(0, 3), dtype=jnp.float32) / width
    pert = (states.astype(jnp.float32) - mean[None, :, :, None]).astype(jnp.bfloat16)
    order = lax.rem(lax.axis_index("member") - jnp.arange(members) + members, members)
    gains = jnp.repeat(transform, BAND, axis=0).reshape(
        strips, rows, members, local_members, width
    )
    gains = jnp.take(gains, order, axis=2)
    gain = jnp.einsum(
        "mjcnxl,jxmnk->kcjxl", pert, gains, preferred_element_type=jnp.float32
    )
    out = mean.transpose(1, 0, 2, 3)[None] + gain
    return out.reshape(width, channels, strips * rows, lanes).astype(jnp.bfloat16)


def local(background, obs_ens, obs_value, obs_precision, obs_row, obs_patch):
    members = lax.axis_size("member")
    regions = lax.axis_size("region")
    obs_rows, width = obs_ens.shape
    capacity = 2 * obs_rows // (members * regions)
    rows = background.shape[2]
    channels = background.shape[1]
    lat_rows = (regions // members) * rows
    lines = [
        column.reshape(obs_rows // LANES, LANES)
        for column in (obs_value, obs_precision, obs_row, obs_patch[:, 0])
    ]
    recv, late, sums = exchange(background, obs_ens.T, lines, capacity)
    for shift in sorted(range(1, members), key=lambda g: (abs(2 * g - members), g)):
        ring = [(k, (k + shift) % members) for k in range(members)]
        late[shift] = lax.ppermute(late[shift], "member", ring)
    transform = band_transforms(total_grams(sums, lat_rows // BAND), width)
    if rows % TILE:
        return apply_plain(recv, late, transform, members)
    wide = widen(transform, members)
    out = apply_early(recv, wide, members, channels, 2)
    return apply_late(late, wide, members, out)


def solution(mesh):
    in_specs = (
        P("member", None, "region", None),
        P(("member", "region"), None),
        P(("member", "region")),
        P(("member", "region")),
        P(("member", "region")),
        P(("member", "region"), None),
    )
    out_specs = P(None, None, "member", "region")
    return jax.shard_map(local, mesh=mesh, in_specs=in_specs, out_specs=out_specs, check_vma=False)
```
